256 devices in a mesh: span: 16 (over x, z_hi), tensor: 16 (over z_lo, y, core).
Axes of the slice: x: 4, y: 4, z: 8 (z_hi: 4, z_lo: 2; z = z_hi * 2 + z_lo), core: 2. Of those that a mesh axis runs over, the one named last changes fastest.
Arguments:
- latents: bfloat16 [2048, 5120], P(('span', 'tensor')), may hold values from -6 to 6
- modulation: float32 [4, 3, 5120], replicated, may hold values from -3 to 3
- w_query: bfloat16 [5120, 4096], P(None, 'tensor'), may hold values from -0.078125 to 0.078125
- w_key: bfloat16 [5120, 4096], P(None, 'tensor'), may hold values from -0.078125 to 0.078125
- w_value: bfloat16 [5120, 4096], P(None, 'tensor'), may hold values from -0.078125 to 0.078125
- w_out: bfloat16 [4096, 5120], P('tensor'), may hold values from -0.5 to 0.5
- cache_k: bfloat16 [4096, 4096], P('span', 'tensor'), may hold values from -800 to 800
- cache_v: bfloat16 [4096, 4096], P('span', 'tensor'), may hold values from -6 to 6
- level_index: int32 [16], P('span'), may hold values from 0 to 3
- rotation: int32 [16], replicated, may hold values from 0 to 15, each once
- cached_tokens: int32 [1], replicated, may hold values from 128 to 4096
Outputs:
- branch: bfloat16 [2048, 5120], P(('span', 'tensor'))
The draws below stay inside these ranges and needn't reach their ends.
All inputs are finite; a program needn't handle non-finite values.
Results may differ from the reference program's by a relative error of at most 0.019.
Values may be sent and summed in bfloat16 or wider, within the bound.
A program may use at most 64 MiB of HBM per device.

```python
import jax
import jax.numpy as jnp
from jax import lax

D = 5120
HEADS = 32
HD = 128
LEVELS = 4
SPAN_TOK = 128
TOKENS = 2048
CACHE_TOK = 4096
INNER = 4096
N_SPAN = 16


def draw_cache_k(key, part):
    base = jnp.clip(jax.random.normal(key, (CACHE_TOK, HEADS * HD), jnp.float32), -6.0, 6.0)
    return base.astype(jnp.bfloat16)


def set_ends(entries, key, smallest, top_value):
    longest = entries.shape.index(max(entries.shape))
    spots = []
    for shift in (0, 1):
        where = [jax.random.randint(jax.random.fold_in(key, axis), (), 0, length) for axis, length in enumerate(entries.shape)]
        where[longest] = (where[longest] + shift) % entries.shape[longest]
        spots.append(tuple(where))
    return entries.at[spots[0]].set(smallest).at[spots[1]].set(top_value)


def block_levels(key, extent, shards, smallest, largest):
    def one(position, blocks):
        draws = jax.random.uniform(jax.random.fold_in(jax.random.fold_in(key, 6), position), (blocks,), jnp.float32, smallest / len(shards), largest / len(shards))
        return jnp.repeat(jnp.exp(draws), extent[position] // blocks).reshape((-1,) + (1,) * (len(extent) - position - 1))

    level = one(*shards[0])
    for cut in shards[1:]:
        level = level * one(*cut)
    return level


def noise(rng, dims, spread, bound, shards=(), held_as=jnp.bfloat16):
    array = spread * jax.random.normal(rng, dims, jnp.float32)
    if shards:
        array = array * block_levels(rng, dims, shards, -0.22, 0.18)
    return jnp.clip(array, -bound, bound).astype(held_as)


def setup_inputs(seed: int = 0) -> dict:
    keys = jax.random.split(jax.random.key(seed), 12)
    latents = noise(keys[0], (TOKENS, D), 1.0, 6.0, ((0, 256),))
    modulation = noise(keys[1], (LEVELS, 3, D), 0.5, 3.0, (), jnp.float32)
    w_query = noise(keys[2], (D, INNER), D ** -0.5, 0.078125, ((1, 16),))
    w_key = noise(keys[3], (D, INNER), D ** -0.5, 0.078125, ((1, 16),))
    w_value = noise(keys[4], (D, INNER), D ** -0.5, 0.078125, ((1, 16),))
    w_out = noise(keys[5], (INNER, D), HD ** -0.5, 0.5, ((0, 16),))
    cache_k = draw_cache_k(jax.random.fold_in(keys[11], 71), 0)
    cache_v = noise(keys[7], (CACHE_TOK, INNER), 1.0, 6.0, ((0, 16), (1, 16)))
    level_index = set_ends(jax.random.randint(keys[8], (N_SPAN,), 0, LEVELS), jax.random.fold_in(keys[8], 1), 0, LEVELS - 1).astype(jnp.int32)
    rotation = jax.random.permutation(keys[9], N_SPAN).astype(jnp.int32)
    cached_tokens = jax.random.randint(keys[10], (1,), SPAN_TOK, CACHE_TOK + 1).astype(jnp.int32)
    return dict(latents=latents, modulation=modulation, w_query=w_query, w_key=w_key, w_value=w_value, w_out=w_out, cache_k=cache_k, cache_v=cache_v, level_index=level_index, rotation=rotation, cached_tokens=cached_tokens)


EPSILON = 1e-06

def reference(latents, modulation, w_query, w_key, w_value, w_out, cache_k, cache_v, level_index, rotation, cached_tokens):
    groups = N_SPAN
    mod_rows = jnp.take(modulation, level_index, axis=0)
    row_data = latents.astype(jnp.float32).reshape(groups, SPAN_TOK, D)
    row_mean = lax.optimization_barrier(jnp.mean(row_data, axis=-1, keepdims=True))
    centred = row_data - row_mean
    row_var = lax.optimization_barrier(jnp.mean(centred * centred, axis=-1, keepdims=True))
    normed = centred * lax.rsqrt(row_var + EPSILON)
    modulated = (normed * (1.0 + mod_rows[:, 1:2, :]) + mod_rows[:, 0:1, :]).astype(jnp.bfloat16).reshape(TOKENS, D)
    queries = jnp.dot(modulated, w_query, preferred_element_type=jnp.float32).astype(jnp.bfloat16)
    keys_new = jnp.dot(modulated, w_key, preferred_element_type=jnp.float32).astype(jnp.bfloat16)
    values_new = jnp.dot(modulated, w_value, preferred_element_type=jnp.float32).astype(jnp.bfloat16)
    order = rotation.astype(jnp.int32)
    live_keys = cached_tokens[0]
    cache_valid = jnp.arange(CACHE_TOK, dtype=jnp.int32) < live_keys
    all_keys = jnp.concatenate([cache_k, keys_new], 0).reshape(-1, HEADS, HD).transpose(1, 0, 2)
    all_values = jnp.concatenate([cache_v, values_new], 0).reshape(-1, HEADS, HD).transpose(1, 0, 2)
    key_group = jnp.arange(TOKENS, dtype=jnp.int32) // SPAN_TOK

    def one_span(span):
        allowed = order[key_group] <= order[span]
        key_valid = jnp.concatenate([cache_valid, allowed])
        q_block = lax.dynamic_slice_in_dim(queries, (span * SPAN_TOK).astype(jnp.int32), SPAN_TOK, 0)
        q_block = q_block.reshape(SPAN_TOK, HEADS, HD).transpose(1, 0, 2)

        def one_head(operands):
            q_head, k_head, v_head = operands
            scores = jnp.dot(q_head, k_head.T, preferred_element_type=jnp.float32) * HD ** (-0.5)
            scores = jnp.where(key_valid[None, :], scores, -1e+30)
            top_score = lax.optimization_barrier(jnp.max(scores, axis=1, keepdims=True))
            weights = jnp.where(key_valid[None, :], jnp.exp(scores - top_score), 0.0)
            summed = jnp.dot(weights.astype(jnp.bfloat16), v_head, preferred_element_type=jnp.float32)
            return summed / lax.optimization_barrier(jnp.sum(weights, axis=1, keepdims=True))
        result = lax.map(one_head, (q_block, all_keys, all_values))
        return result.transpose(1, 0, 2).reshape(SPAN_TOK, HEADS * HD).astype(jnp.bfloat16)
    attended = lax.map(one_span, jnp.arange(groups, dtype=jnp.int32)).reshape(TOKENS, HEADS * HD)
    projection = jnp.dot(attended, w_out, preferred_element_type=jnp.float32).reshape(groups, SPAN_TOK, D)
    return (mod_rows[:, 2:3, :] * projection).astype(jnp.bfloat16).reshape(TOKENS, D)
```

```python
import functools

import jax
import jax.numpy as jnp
from jax import lax
from jax.experimental import pallas as pl
from jax.experimental.pallas import tpu as pltpu
from jax.sharding import PartitionSpec as P

HD = 128
EPSILON = 1e-06
NEG = -1e30
MESH = pl.DeviceIdType.MESH
F32 = jnp.float32
BF16 = jnp.bfloat16
SCALE2 = HD**-0.5 * 1.4426950408889634

D = 5120
HALF = D // 2
XN, ZN, YN = 4, 4, 4
CHIPS = 8
ROWS = 8
CACHE = 256
SPAN = 128
KEYS = XN * (CACHE + SPAN)
CHIP_STEPS = ((0, 1), (0, 3), (1, 0), (1, 1), (1, 3), (0, 2), (1, 2))
GROUPS = ((0, 0), (1, 0), (0, 1), (1, 1))


def kernel(
    latents, modulation, w_query, w_key, w_value, w_out, cache_k, cache_v, level_index, rotation, cached_tokens,
    out_ref,
    x_buf, lhs, mod, scale_rows, shift_rows, w_in, w_o, ck, cv, nk, nv, qb, bias, scores,
    o_send, o_recv, s_send, s_recv, att, p_send, p_recv,
    load_sem, lat_send, lat_recv, fwd_send, ck_send, ck_recv, q_send, q_recv, kv_send, kv_recv,
    wo_send, wo_recv, ot_send, ot_recv, st_send, st_recv, pr_send, pr_recv,
):
    span = lax.axis_index("span")
    tensor = lax.axis_index("tensor")
    x = span // ZN
    zh = span % ZN
    zl = tensor // 8
    y = (tensor // 2) % YN
    core = tensor % 2
    chip = zl * YN + y
    other = 1 - core

    def chip_at(dl, dy):
        return ((zl + dl) % 2) * YN + (y + dy) % YN

    def chip_device(dl, dy, c):
        return (span, chip_at(dl, dy) * 2 + c)

    sibling = (span, chip * 2 + other)

    def x_device(dx):
        return (((x + dx) % XN) * ZN + zh, tensor)

    def z_device(dz, c):
        return (x * ZN + (zh + dz) % ZN, chip * 2 + c)

    def remote(src, dst, send, recv, device):
        return pltpu.make_async_remote_copy(
            src_ref=src, dst_ref=dst, send_sem=send, recv_sem=recv, device_id=device, device_id_type=MESH
        )

    loads = [
        pltpu.make_async_copy(latents, x_buf.at[tensor], load_sem.at[0]),
        pltpu.make_async_copy(cache_k, ck.at[x], load_sem.at[1]),
        pltpu.make_async_copy(cache_v, cv.at[x], load_sem.at[2]),
        pltpu.make_async_copy(modulation, mod, load_sem.at[3]),
        pltpu.make_async_copy(w_query, w_in.at[0], load_sem.at[4]),
        pltpu.make_async_copy(w_key, w_in.at[1], load_sem.at[5]),
        pltpu.make_async_copy(w_value, w_in.at[2], load_sem.at[6]),
        pltpu.make_async_copy(w_out, w_o.at[core], load_sem.at[7]),
    ]
    for copy in loads:
        copy.start()

    barrier = pltpu.get_barrier_semaphore()
    peers = [sibling]
    peers += [chip_device(dl, dy, core) for dl, dy in CHIP_STEPS]
    peers += [x_device(dx) for dx in (1, 2, 3)]
    peers += [z_device(dz, c) for dz in (1, 2, 3) for c in (0, 1)]
    for device in peers:
        pl.semaphore_signal(barrier, inc=1, device_id=device, device_id_type=MESH)

    live = cached_tokens[0]
    lanes = lax.broadcasted_iota(jnp.int32, (ZN, CACHE), 1)
    for xk in range(XN):
        slots = lanes + (xk * ZN + zh) * CACHE
        bias[:, xk * CACHE : (xk + 1) * CACHE] = jnp.where(slots < live, 0.0, NEG)
    for zq in range(ZN):
        order_q = rotation[x * ZN + zq]
        for xk in range(XN):
            seen = jnp.where(rotation[xk * ZN + zh] <= order_q, 0.0, NEG)
            start = XN * CACHE + xk * SPAN
            bias[zq : zq + 1, start : start + SPAN] = jnp.full((1, SPAN), seen, F32)

    loads[0].wait()
    pl.semaphore_wait(barrier, len(peers))

    waits = []

    def send(src, dst, send_sem, recv_sem, device):
        copy = remote(src, dst, send_sem, recv_sem, device)
        copy.start()
        waits.append(copy)

    own_rows = x_buf.at[tensor]
    for k, (dl, dy) in enumerate(CHIP_STEPS):
        send(own_rows, own_rows, lat_send.at[k], lat_recv.at[tensor], chip_device(dl, dy, core))
    send(own_rows, own_rows, fwd_send.at[7], lat_recv.at[tensor], sibling)

    loads[1].wait()
    loads[2].wait()
    for k, dx in enumerate((1, 3, 2)):
        send(ck.at[x], ck.at[x], ck_send.at[2 * k], ck_recv.at[2 * x], x_device(dx))
        send(cv.at[x], cv.at[x], ck_send.at[2 * k + 1], ck_recv.at[2 * x + 1], x_device(dx))

    loads[3].wait()
    level = level_index[0]
    shift_rows[...] = jnp.broadcast_to(mod[level, 0:1, :], (ROWS, D))
    scale_rows[...] = jnp.broadcast_to(1.0 + mod[level, 1:2, :], (ROWS, D))

    def arrived(index):
        remote(x_buf.at[index], x_buf.at[index], lat_send.at[0], lat_recv.at[index], sibling).wait_recv()

    def normalised(index):
        row_data = x_buf[index].astype(F32)
        mean = jnp.sum(row_data, axis=1, keepdims=True) * (1.0 / D)
        centred = row_data - mean
        var = jnp.sum(centred * centred, axis=1, keepdims=True) * (1.0 / D)
        return centred * lax.rsqrt(var + EPSILON) * scale_rows[...] + shift_rows[...]

    def normalise_pair(first_chip, c):
        rows = jnp.concatenate(
            [normalised(first_chip * 2 + c), normalised((first_chip + 1) * 2 + c)], axis=0
        )
        start = pl.multiple_of(c * (CHIPS * ROWS) + first_chip * ROWS, 16)
        lhs[pl.ds(start, 16), :] = rows.astype(BF16)

    def group_chip(dl, dp):
        return ((zl + dl) % 2) * YN + ((y // 2 + dp) % 2) * 2

    def sibling_pair(first):
        arrived(first * 2 + other)
        arrived((first + 1) * 2 + other)
        normalise_pair(first, other)

    for g, (dl, dp) in enumerate(GROUPS):
        first = group_chip(dl, dp)
        if g == 0:
            mate = first + (1 - y % 2)
            members = [mate]
        else:
            members = [first, first + 1]
        for m, member in enumerate(members):
            arrived(member * 2 + core)
            piece = x_buf.at[member * 2 + core]
            k = 0 if g == 0 else 2 * g - 1 + m
            send(piece, piece, fwd_send.at[k], lat_recv.at[member * 2 + core], sibling)
        normalise_pair(first, core)
        if g > 0:
            sibling_pair(group_chip(*GROUPS[g - 1]))
    sibling_pair(group_chip(*GROUPS[3]))

    def project(which):
        return jnp.dot(lhs[...], w_in[which], preferred_element_type=F32).astype(BF16)

    loads[4].wait()
    queries = project(0)
    for h in range(2):
        qb[h, zh] = queries[:, h * HD : (h + 1) * HD]
    for h in range(2):
        for k, dz in enumerate((2, 1, 3)):
            send(qb.at[h, zh], qb.at[h, zh], q_send.at[3 * h + k], q_recv.at[4 * h + zh], z_device(dz, core))

    def send_rows(buf, v, h):
        for k, dx in enumerate((1, 3, 2)):
            slot = 4 * v + 2 * h
            send(
                buf.at[h, x], buf.at[h, x], kv_send.at[3 * (2 * v + h) + k], kv_recv.at[4 * (2 * v + h) + x], x_device(dx)
            )

    loads[5].wait()
    keys = project(1)
    for h in range(2):
        nk[h, x] = keys[:, h * HD : (h + 1) * HD]
    send_rows(nk, 0, 0)
    loads[6].wait()
    values = project(2)
    for h in range(2):
        nv[h, x] = values[:, h * HD : (h + 1) * HD]
    send_rows(nv, 1, 0)
    send_rows(nk, 0, 1)
    send_rows(nv, 1, 1)
    loads[7].wait()
    send(w_o.at[core], w_o.at[core], wo_send, wo_recv, sibling)

    eye = lax.broadcasted_iota(jnp.int32, (SPAN, SPAN), 0) == lax.broadcasted_iota(jnp.int32, (SPAN, SPAN), 1)

    def key_chunk(h, j):
        if j < XN:
            return ck[j, :, h * HD : (h + 1) * HD]
        j -= XN
        return nk[h, 2 * j : 2 * j + 2].reshape(2 * SPAN, HD)

    def value_chunk(h, j):
        if j < XN:
            return cv[j, :, h * HD : (h + 1) * HD]
        j -= XN
        return nv[h, 2 * j : 2 * j + 2].reshape(2 * SPAN, HD)

    chunks = KEYS // 256

    def attend(h, zq):
        q = qb[h, zq]
        top = None
        for j in range(chunks):
            s = lax.dot_general(q, key_chunk(h, j), (((1,), (1,)), ((), ())), preferred_element_type=F32)
            s = s + bias[pl.ds(zq, 1), j * 256 : (j + 1) * 256]
            scores[:, j * 256 : (j + 1) * 256] = s
            best = jnp.maximum(s[:, :128], s[:, 128:])
            top = best if top is None else jnp.maximum(top, best)
        row_max = jnp.max(top, axis=1, keepdims=True)
        total = jnp.zeros((SPAN, 128), F32)
        acc = jnp.zeros((SPAN, HD), F32)
        for j in range(chunks):
            p = jnp.exp2((scores[:, j * 256 : (j + 1) * 256] - row_max) * SCALE2)
            total = total + (p[:, :128] + p[:, 128:])
            acc = acc + jnp.dot(p.astype(BF16), value_chunk(h, j), preferred_element_type=F32)
        row_sum = jnp.sum(total, axis=1, keepdims=True)
        lse = row_max * SCALE2 + jnp.log2(row_sum)
        part = (acc / row_sum).astype(BF16)
        stat = jnp.sum(jnp.where(eye, lse, 0.0), axis=0, keepdims=True)
        return part, stat

    for h in range(2):
        for dx in (1, 3, 2):
            xk = (x + dx) % XN
            if h == 0:
                remote(ck.at[xk], ck.at[xk], ck_send.at[0], ck_recv.at[2 * xk], sibling).wait_recv()
                remote(cv.at[xk], cv.at[xk], ck_send.at[0], ck_recv.at[2 * xk + 1], sibling).wait_recv()
            remote(nk.at[h, xk], nk.at[h, xk], kv_send.at[0], kv_recv.at[4 * h + xk], sibling).wait_recv()
            remote(nv.at[h, xk], nv.at[h, xk], kv_send.at[0], kv_recv.at[8 + 4 * h + xk], sibling).wait_recv()
        for k, dz in enumerate((1, 3, 2, 0)):
            zq = (zh + dz) % ZN
            if dz:
                remote(qb.at[h, zq], qb.at[h, zq], q_send.at[0], q_recv.at[4 * h + zq], sibling).wait_recv()
            part, stat = attend(h, zq)
            rows = CHIPS * ROWS
            s_send[h, zq] = jnp.broadcast_to(stat, (8, SPAN))
            o_send[h, zq, 0] = part[:rows]
            o_send[h, zq, 1] = part[rows:]
            for c in range(2):
                if dz:
                    n = 6 * h + 2 * k + c
                    slot = 8 * h + 2 * zh
                    device = z_device(dz, c)
                    send(o_send.at[h, zq, c], o_recv.at[h, zh, core], ot_send.at[n], ot_recv.at[slot + core], device)
                    send(s_send.at[h, zq], s_recv.at[h, zh, core], st_send.at[n], st_recv.at[slot + core], device)
            if dz == 0:
                send(
                    o_send.at[h, zq, other], o_recv.at[h, zh, core], ot_send.at[12 + h],
                    ot_recv.at[8 * h + 2 * zh + core], sibling,
                )
                send(
                    s_send.at[h, zq], s_recv.at[h, zh, core], st_send.at[12 + h],
                    st_recv.at[8 * h + 2 * zh + core], sibling,
                )
                o_recv[h, zh, core] = o_send[h, zh, core]
                s_recv[h, zh, core] = s_send[h, zh]

    rows = CHIPS * ROWS
    mine = lax.broadcasted_iota(jnp.int32, (rows, SPAN), 1) == core * rows + lax.broadcasted_iota(
        jnp.int32, (rows, SPAN), 0
    )
    for h in range(2):
        for dz in (0, 1, 3, 2):
            zs = (zh + dz) % ZN
            for dc in range(2):
                cs = (core + dc) % 2
                if dz or dc:
                    slot = 8 * h + 2 * zs + cs
                    remote(o_recv.at[h, zs, cs], o_recv.at[h, zs, cs], ot_send.at[0], ot_recv.at[slot], sibling).wait_recv()
                    remote(s_recv.at[h, zs, cs], s_recv.at[h, zs, cs], st_send.at[0], st_recv.at[slot], sibling).wait_recv()
        for cs in range(2):
            lses = [
                jnp.sum(jnp.where(mine, s_recv[h, zs, cs, 0:1, :], 0.0), axis=1, keepdims=True) for zs in range(ZN)
            ]
            best = jnp.maximum(jnp.maximum(lses[0], lses[1]), jnp.maximum(lses[2], lses[3]))
            shares = [jnp.exp2(value - best) for value in lses]
            whole = shares[0] + shares[1] + shares[2] + shares[3]
            summed = sum(shares[zs] * o_recv[h, zs, cs].astype(F32) for zs in range(ZN))
            att[:, (2 * cs + h) * HD : (2 * cs + h + 1) * HD] = (summed / whole).astype(BF16)

    remote(w_o.at[other], w_o.at[other], wo_send, wo_recv, sibling).wait_recv()
    step = 512
    for half in range(2):

        @pl.loop(0, HALF // step)
        def _(n):
            cols = pl.ds(pl.multiple_of(half * HALF + n * step, step), step)
            value = jnp.dot(att[:, : 2 * HD], w_o[0, :, cols], preferred_element_type=F32) + jnp.dot(
                att[:, 2 * HD :], w_o[1, :, cols], preferred_element_type=F32
            )
            p_send[:, :, cols] = value.reshape(CHIPS, ROWS, step).astype(BF16)

        cols = pl.ds(half * HALF, HALF)
        for k, (dl, dy) in enumerate(CHIP_STEPS):
            send(
                p_send.at[chip_at(dl, dy), :, cols], p_recv.at[chip, :, cols], pr_send.at[7 * half + k],
                pr_recv.at[8 * half + chip], chip_device(dl, dy, core),
            )

    gate = mod[level, 2:3, :]
    for half in range(2):
        cols = pl.ds(half * HALF, HALF)
        total = p_send[chip, :, cols].astype(F32)
        for dl, dy in CHIP_STEPS:
            source = chip_at(dl, dy)
            remote(
                p_recv.at[source, :, cols], p_recv.at[source, :, cols], pr_send.at[0], pr_recv.at[8 * half + source],
                sibling,
            ).wait_recv()
            total = total + p_recv[source, :, cols].astype(F32)
        out_ref[:, half * HALF : (half + 1) * HALF] = (gate[:, half * HALF : (half + 1) * HALF] * total).astype(BF16)

    for copy in waits:
        copy.wait_send()


def body(
    latents, modulation, w_query, w_key, w_value, w_out, cache_k, cache_v, level_index, rotation, cached_tokens
):
    anywhere = pl.BlockSpec(memory_space=pl.ANY)
    smem = pl.BlockSpec(memory_space=pltpu.SMEM)
    dma = pltpu.SemaphoreType.DMA
    rows = CHIPS * ROWS
    return pl.pallas_call(
        kernel,
        out_shape=jax.ShapeDtypeStruct((ROWS, D), BF16),
        in_specs=[anywhere] * 8 + [smem] * 3,
        out_specs=pl.BlockSpec(memory_space=pltpu.VMEM),
        scratch_shapes=[
            pltpu.VMEM((16, ROWS, D), BF16),
            pltpu.VMEM((SPAN, D), BF16),
            pltpu.VMEM((4, 3, D), F32),
            pltpu.VMEM((ROWS, D), F32),
            pltpu.VMEM((ROWS, D), F32),
            pltpu.VMEM((3, D, 2 * HD), BF16),
            pltpu.VMEM((2, 2 * HD, D), BF16),
            pltpu.VMEM((XN, CACHE, 2 * HD), BF16),
            pltpu.VMEM((XN, CACHE, 2 * HD), BF16),
            pltpu.VMEM((2, XN, SPAN, HD), BF16),
            pltpu.VMEM((2, XN, SPAN, HD), BF16),
            pltpu.VMEM((2, ZN, SPAN, HD), BF16),
            pltpu.VMEM((ZN, KEYS), F32),
            pltpu.VMEM((SPAN, KEYS), F32),
            pltpu.VMEM((2, ZN, 2, rows, HD), BF16),
            pltpu.VMEM((2, ZN, 2, rows, HD), BF16),
            pltpu.VMEM((2, ZN, 8, SPAN), F32),
            pltpu.VMEM((2, ZN, 2, 8, SPAN), F32),
            pltpu.VMEM((rows, 4 * HD), BF16),
            pltpu.VMEM((CHIPS, ROWS, D), BF16),
            pltpu.VMEM((CHIPS, ROWS, D), BF16),
            dma((8,)),
            dma((7,)),
            dma((16,)),
            dma((8,)),
            dma((6,)),
            dma((8,)),
            dma((6,)),
            dma((8,)),
            dma((12,)),
            dma((16,)),
            dma(()),
            dma(()),
            dma((14,)),
            dma((16,)),
            dma((14,)),
            dma((16,)),
            dma((14,)),
            dma((16,)),
        ],
        compiler_params=pltpu.CompilerParams(
            collective_id=0, has_side_effects=True, vmem_limit_bytes=60 * 1024 * 1024
        ),
        name="attention_step",
    )(latents, modulation, w_query, w_key, w_value, w_out, cache_k, cache_v, level_index, rotation, cached_tokens)


def solution(mesh):
    placed = (
        P(("span", "tensor"), None),
        P(),
        P(None, "tensor"),
        P(None, "tensor"),
        P(None, "tensor"),
        P("tensor", None),
        P("span", "tensor"),
        P("span", "tensor"),
        P("span"),
        P(),
        P(),
    )
    return jax.shard_map(
        body, mesh=mesh, in_specs=placed, out_specs=P(("span", "tensor"), None), check_vma=False
    )
```

```python
import functools

import jax
import jax.numpy as jnp
from jax import lax
from jax.experimental import pallas as pl
from jax.experimental.pallas import tpu as pltpu
from jax.sharding import PartitionSpec as P

HD = 128
EPSILON = 1e-06
NEG = -1e30
MESH = pl.DeviceIdType.MESH
F32 = jnp.float32
BF16 = jnp.bfloat16
SCALE2 = HD**-0.5 * 1.4426950408889634

D = 5120
HALF = D // 2
XN, ZN, YN = 4, 4, 4
CHIPS = 8
ROWS = 8
CACHE = 256
SPAN = 128
KEYS = XN * (CACHE + SPAN)
CHIP_STEPS = ((0, 1), (0, 3), (1, 0), (1, 1), (1, 3), (0, 2), (1, 2))
PARTS = 4
WIDTH = D // PARTS
GROUPS = ((0, 0), (1, 0), (0, 1), (1, 1))


def kernel(
    latents, modulation, w_query, w_key, w_value, w_out, cache_k, cache_v, level_index, rotation, cached_tokens,
    out_ref,
    level_s, rot_s, live_s, x_buf, lhs, mod, scale_rows, shift_rows, w_in, w_o, ck, cv, nk, nv, qb, slot_bias, span_bias, v_raw, scores,
    o_send, o_recv, s_send, s_recv, att, p_send, p_recv,
    load_sem, lat_send, lat_recv, fwd_send, ck_send, ck_recv, q_send, q_recv, kv_send, kv_recv,
    wo_send, wo_recv, ot_send, ot_recv, st_send, st_recv, pr_send, pr_recv,
):
    span = lax.axis_index("span")
    tensor = lax.axis_index("tensor")
    x = span // ZN
    zh = span % ZN
    zl = tensor // 8
    y = (tensor // 2) % YN
    core = tensor % 2
    chip = zl * YN + y
    other = 1 - core

    def chip_at(dl, dy):
        return ((zl + dl) % 2) * YN + (y + dy) % YN

    def chip_device(dl, dy, c):
        return (span, chip_at(dl, dy) * 2 + c)

    sibling = (span, chip * 2 + other)

    def x_device(dx):
        return (((x + dx) % XN) * ZN + zh, tensor)

    def z_device(dz, c):
        return (x * ZN + (zh + dz) % ZN, chip * 2 + c)

    def remote(src, dst, send, recv, device):
        return pltpu.make_async_remote_copy(
            src_ref=src, dst_ref=dst, send_sem=send, recv_sem=recv, device_id=device, device_id_type=MESH
        )

    scalars = [
        pltpu.make_async_copy(level_index, level_s, load_sem.at[8]),
        pltpu.make_async_copy(rotation, rot_s, load_sem.at[9]),
        pltpu.make_async_copy(cached_tokens, live_s, load_sem.at[10]),
    ]
    loads = [
        pltpu.make_async_copy(latents, x_buf.at[tensor], load_sem.at[0]),
        pltpu.make_async_copy(cache_k, ck.at[x], load_sem.at[1]),
        pltpu.make_async_copy(cache_v, v_raw, load_sem.at[2]),
        pltpu.make_async_copy(modulation, mod, load_sem.at[3]),
        pltpu.make_async_copy(w_query, w_in.at[0], load_sem.at[4]),
        pltpu.make_async_copy(w_key, w_in.at[1], load_sem.at[5]),
        pltpu.make_async_copy(w_value, w_in.at[2], load_sem.at[6]),
        pltpu.make_async_copy(w_out, w_o.at[core], load_sem.at[7]),
    ]
    for copy in loads[:1] + scalars + loads[1:]:
        copy.start()

    barrier = pltpu.get_barrier_semaphore()
    peers = [sibling]
    peers += [chip_device(dl, dy, core) for dl, dy in CHIP_STEPS]
    peers += [x_device(dx) for dx in (1, 2, 3)]
    peers += [z_device(dz, c) for dz in (1, 2, 3) for c in (0, 1)]
    for device in peers:
        pl.semaphore_signal(barrier, inc=1, device_id=device, device_id_type=MESH)

    for copy in scalars:
        copy.wait()
    live = live_s[0]
    level = level_s[0]
    slot = lax.broadcasted_iota(jnp.int32, (CACHE, SPAN), 0)
    for xk in range(XN):
        base = (xk * ZN + zh) * CACHE
        slot_bias[xk * CACHE : (xk + 1) * CACHE] = jnp.where(slot + base < live, 0.0, NEG)
    for zq in range(ZN):
        order_q = rot_s[x * ZN + zq]
        for xk in range(XN):
            seen = jnp.where(rot_s[xk * ZN + zh] <= order_q, 0.0, NEG)
            span_bias[zq, xk] = jnp.full((ROWS, SPAN), seen, F32)

    loads[0].wait()
    pl.semaphore_wait(barrier, len(peers))

    waits = []

    def send(src, dst, send_sem, recv_sem, device):
        copy = remote(src, dst, send_sem, recv_sem, device)
        copy.start()
        waits.append(copy)

    own_rows = x_buf.at[tensor]
    for k, (dl, dy) in enumerate(CHIP_STEPS):
        send(own_rows, own_rows, lat_send.at[k], lat_recv.at[tensor], chip_device(dl, dy, core))
    send(own_rows, own_rows, fwd_send.at[7], lat_recv.at[tensor], sibling)

    loads[1].wait()
    loads[2].wait()
    cv[x] = v_raw[...].T
    for k, dx in enumerate((1, 3, 2)):
        send(ck.at[x], ck.at[x], ck_send.at[2 * k], ck_recv.at[2 * x], x_device(dx))
        send(cv.at[x], cv.at[x], ck_send.at[2 * k + 1], ck_recv.at[2 * x + 1], x_device(dx))

    loads[3].wait()
    shift_rows[...] = jnp.broadcast_to(mod[0, pl.ds(level, 1), :], (ROWS, D))
    scale_rows[...] = jnp.broadcast_to(1.0 + mod[1, pl.ds(level, 1), :], (ROWS, D))

    def arrived(index):
        remote(x_buf.at[index], x_buf.at[index], lat_send.at[0], lat_recv.at[index], sibling).wait_recv()

    def normalised(index):
        row_data = x_buf[index].astype(F32)
        mean = jnp.sum(row_data, axis=1, keepdims=True) * (1.0 / D)
        centred = row_data - mean
        var = jnp.sum(centred * centred, axis=1, keepdims=True) * (1.0 / D)
        return centred * lax.rsqrt(var + EPSILON) * scale_rows[...] + shift_rows[...]

    def normalise_pair(first_chip, c):
        rows = jnp.concatenate(
            [normalised(first_chip * 2 + c), normalised((first_chip + 1) * 2 + c)], axis=0
        )
        start = pl.multiple_of(c * (CHIPS * ROWS) + first_chip * ROWS, 16)
        lhs[pl.ds(start, 16), :] = rows.astype(BF16)

    def group_chip(dl, dp):
        return ((zl + dl) % 2) * YN + ((y // 2 + dp) % 2) * 2

    def sibling_pair(first):
        arrived(first * 2 + other)
        arrived((first + 1) * 2 + other)
        normalise_pair(first, other)

    for g, (dl, dp) in enumerate(GROUPS):
        first = group_chip(dl, dp)
        if g == 0:
            mate = first + (1 - y % 2)
            members = [mate]
        else:
            members = [first, first + 1]
        for m, member in enumerate(members):
            arrived(member * 2 + core)
            piece = x_buf.at[member * 2 + core]
            k = 0 if g == 0 else 2 * g - 1 + m
            send(piece, piece, fwd_send.at[k], lat_recv.at[member * 2 + core], sibling)
        normalise_pair(first, core)
        if g > 0:
            sibling_pair(group_chip(*GROUPS[g - 1]))
    sibling_pair(group_chip(*GROUPS[3]))

    def project(which):
        sums = [None, None]
        for n in range(D // 256):
            depth = slice(n // 2 * 256 + n % 2 * HALF, (n // 2 + 1) * 256 + n % 2 * HALF)
            part = jnp.dot(lhs[:, depth], w_in[which, depth], preferred_element_type=F32)
            sums[n % 2] = part if sums[n % 2] is None else sums[n % 2] + part
        return (sums[0] + sums[1]).astype(BF16)

    loads[4].wait()
    queries = project(0)
    for h in range(2):
        qb[h, zh] = queries[:, h * HD : (h + 1) * HD]
    for h in range(2):
        for k, dz in enumerate((2, 1, 3)):
            send(qb.at[h, zh], qb.at[h, zh], q_send.at[3 * h + k], q_recv.at[4 * h + zh], z_device(dz, core))

    def send_rows(buf, v, h):
        for k, dx in enumerate((1, 3, 2)):
            send(
                buf.at[h, x], buf.at[h, x], kv_send.at[3 * (2 * v + h) + k], kv_recv.at[4 * (2 * v + h) + x], x_device(dx)
            )

    loads[5].wait()
    keys = project(1)
    for h in range(2):
        nk[h, x] = keys[:, h * HD : (h + 1) * HD]
    send_rows(nk, 0, 0)
    loads[6].wait()
    values = project(2)
    for h in range(2):
        nv[h, x] = values[:, h * HD : (h + 1) * HD].T
    send_rows(nv, 1, 0)
    send_rows(nk, 0, 1)
    send_rows(nv, 1, 1)
    loads[7].wait()
    send(w_o.at[core], w_o.at[core], wo_send, wo_recv, sibling)

    def key_chunk(h, j):
        if j < XN:
            return ck[j, :, h * HD : (h + 1) * HD]
        j -= XN
        return nk[h, 2 * j : 2 * j + 2].reshape(2 * SPAN, HD)

    def value_chunk(h, j):
        if j < XN:
            return cv[j, h * HD : (h + 1) * HD, :]
        j -= XN
        return jnp.concatenate([nv[h, 2 * j], nv[h, 2 * j + 1]], axis=1)

    def mask_chunk(zqs, j):
        if j < XN:
            tile = slot_bias[j * CACHE : (j + 1) * CACHE]
            return jnp.concatenate([tile] * len(zqs), axis=1)
        j -= XN
        rows = []
        for xk in (2 * j, 2 * j + 1):
            tile = jnp.concatenate([span_bias[zq, xk] for zq in zqs], axis=1)
            rows.append(jnp.broadcast_to(tile[None], (SPAN // ROWS, *tile.shape)).reshape(SPAN, -1))
        return jnp.concatenate(rows, axis=0)

    chunks = KEYS // 256

    def attend(h, zqs):
        width = len(zqs) * SPAN
        q = jnp.concatenate([qb[h, zq] for zq in zqs], axis=0)
        top = None
        for j in range(chunks):
            s = lax.dot_general(key_chunk(h, j), q, (((1,), (1,)), ((), ())), preferred_element_type=F32)
            s = s + mask_chunk(zqs, j)
            scores[j * 256 : (j + 1) * 256] = s
            best = jnp.max(s.reshape(256 // ROWS, ROWS, width), axis=0)
            top = best if top is None else jnp.maximum(top, best)
        top = jnp.max(top, axis=0, keepdims=True)
        acc = total = None
        for j in range(chunks):
            p = jnp.exp2((scores[j * 256 : (j + 1) * 256] - top) * SCALE2)
            share = jnp.sum(p.reshape(256 // ROWS, ROWS, width), axis=0)
            part = jnp.dot(value_chunk(h, j), p.astype(BF16), preferred_element_type=F32)
            total = share if total is None else total + share
            acc = part if acc is None else acc + part
        total = jnp.sum(total, axis=0, keepdims=True)
        lse = top * SCALE2 + jnp.log2(total)
        acc = acc / total
        out = []
        for n in range(len(zqs)):
            cols = slice(n * SPAN, (n + 1) * SPAN)
            out.append((acc[:, cols].T.astype(BF16), lse[:, cols]))
        return out

    for h in range(2):
        for dx in (1, 3, 2):
            xk = (x + dx) % XN
            if h == 0:
                remote(ck.at[xk], ck.at[xk], ck_send.at[0], ck_recv.at[2 * xk], sibling).wait_recv()
                remote(cv.at[xk], cv.at[xk], ck_send.at[0], ck_recv.at[2 * xk + 1], sibling).wait_recv()
            remote(nk.at[h, xk], nk.at[h, xk], kv_send.at[0], kv_recv.at[4 * h + xk], sibling).wait_recv()
            remote(nv.at[h, xk], nv.at[h, xk], kv_send.at[0], kv_recv.at[8 + 4 * h + xk], sibling).wait_recv()
        results = []
        for k, dz in enumerate((1, 3, 2, 0)):
            zq = (zh + dz) % ZN
            if k % 2 == 0:
                pair = [1, 3] if k == 0 else [2, 0]
                zqs = [(zh + d) % ZN for d in pair]
                for d, z in zip(pair, zqs):
                    if d:
                        remote(qb.at[h, z], qb.at[h, z], q_send.at[0], q_recv.at[4 * h + z], sibling).wait_recv()
                results += attend(h, zqs)
            part, stat = results[k]
            rows = CHIPS * ROWS
            s_send[h, zq] = jnp.broadcast_to(stat, (8, SPAN))
            o_send[h, zq, 0] = part[:rows]
            o_send[h, zq, 1] = part[rows:]
            for c in range(2):
                if dz:
                    n = 6 * h + 2 * k + c
                    slot = 8 * h + 2 * zh
                    device = z_device(dz, c)
                    send(o_send.at[h, zq, c], o_recv.at[h, zh, core], ot_send.at[n], ot_recv.at[slot + core], device)
                    send(s_send.at[h, zq], s_recv.at[h, zh, core], st_send.at[n], st_recv.at[slot + core], device)
            if dz == 0:
                send(
                    o_send.at[h, zq, other], o_recv.at[h, zh, core], ot_send.at[12 + h],
                    ot_recv.at[8 * h + 2 * zh + core], sibling,
                )
                send(
                    s_send.at[h, zq], s_recv.at[h, zh, core], st_send.at[12 + h],
                    st_recv.at[8 * h + 2 * zh + core], sibling,
                )
                o_recv[h, zh, core] = o_send[h, zh, core]
                s_recv[h, zh, core] = s_send[h, zh]

    rows = CHIPS * ROWS
    mine = lax.broadcasted_iota(jnp.int32, (rows, SPAN), 1) == core * rows + lax.broadcasted_iota(
        jnp.int32, (rows, SPAN), 0
    )
    for h in range(2):
        for dz in (0, 1, 3, 2):
            zs = (zh + dz) % ZN
            for dc in range(2):
                cs = (core + dc) % 2
                if dz or dc:
                    slot = 8 * h + 2 * zs + cs
                    remote(o_recv.at[h, zs, cs], o_recv.at[h, zs, cs], ot_send.at[0], ot_recv.at[slot], sibling).wait_recv()
                    remote(s_recv.at[h, zs, cs], s_recv.at[h, zs, cs], st_send.at[0], st_recv.at[slot], sibling).wait_recv()
        for cs in range(2):
            lses = [
                jnp.sum(jnp.where(mine, s_recv[h, zs, cs, 0:1, :], 0.0), axis=1, keepdims=True) for zs in range(ZN)
            ]
            best = jnp.maximum(jnp.maximum(lses[0], lses[1]), jnp.maximum(lses[2], lses[3]))
            shares = [jnp.exp2(value - best) for value in lses]
            whole = shares[0] + shares[1] + shares[2] + shares[3]
            summed = sum(shares[zs] * o_recv[h, zs, cs].astype(F32) for zs in range(ZN))
            att[:, (2 * cs + h) * HD : (2 * cs + h + 1) * HD] = (summed / whole).astype(BF16)

    remote(w_o.at[other], w_o.at[other], wo_send, wo_recv, sibling).wait_recv()
    for part in range(PARTS):
        cols = pl.ds(part * WIDTH, WIDTH)
        value = jnp.dot(att[:, : 2 * HD], w_o[0, :, cols], preferred_element_type=F32) + jnp.dot(
            att[:, 2 * HD :], w_o[1, :, cols], preferred_element_type=F32
        )
        p_send[:, :, cols] = value.reshape(CHIPS, ROWS, WIDTH).astype(BF16)
        for k, (dl, dy) in enumerate(CHIP_STEPS):
            send(
                p_send.at[chip_at(dl, dy), :, cols], p_recv.at[chip, :, cols], pr_send.at[7 * part + k],
                pr_recv.at[8 * part + chip], chip_device(dl, dy, core),
            )

    gate = mod[2, pl.ds(level, 1), :]
    for part in range(PARTS):
        cols = pl.ds(part * WIDTH, WIDTH)
        total = p_send[chip, :, cols].astype(F32)
        for dl, dy in CHIP_STEPS:
            source = chip_at(dl, dy)
            remote(
                p_recv.at[source, :, cols], p_recv.at[source, :, cols], pr_send.at[0], pr_recv.at[8 * part + source],
                sibling,
            ).wait_recv()
            total = total + p_recv[source, :, cols].astype(F32)
        out_ref[:, cols] = (gate[:, part * WIDTH : (part + 1) * WIDTH] * total).astype(BF16)

    for copy in waits:
        copy.wait_send()


def body(
    latents, modulation, w_query, w_key, w_value, w_out, cache_k, cache_v, level_index, rotation, cached_tokens
):
    anywhere = pl.BlockSpec(memory_space=pltpu.HBM)
    dma = pltpu.SemaphoreType.DMA
    rows = CHIPS * ROWS
    return pl.pallas_call(
        kernel,
        out_shape=jax.ShapeDtypeStruct((ROWS, D), BF16),
        in_specs=[anywhere] * 11,
        out_specs=pl.BlockSpec(memory_space=pltpu.VMEM),
        scratch_shapes=[
            pltpu.SMEM((1,), jnp.int32),
            pltpu.SMEM((16,), jnp.int32),
            pltpu.SMEM((1,), jnp.int32),
            pltpu.VMEM((16, ROWS, D), BF16),
            pltpu.VMEM((SPAN, D), BF16),
            pltpu.VMEM((3, 4, D), F32),
            pltpu.VMEM((ROWS, D), F32),
            pltpu.VMEM((ROWS, D), F32),
            pltpu.VMEM((3, D, 2 * HD), BF16),
            pltpu.VMEM((2, 2 * HD, D), BF16),
            pltpu.VMEM((XN, CACHE, 2 * HD), BF16),
            pltpu.VMEM((XN, 2 * HD, CACHE), BF16),
            pltpu.VMEM((2, XN, SPAN, HD), BF16),
            pltpu.VMEM((2, XN, HD, SPAN), BF16),
            pltpu.VMEM((2, ZN, SPAN, HD), BF16),
            pltpu.VMEM((XN * CACHE, SPAN), F32),
            pltpu.VMEM((ZN, XN, ROWS, SPAN), F32),
            pltpu.VMEM((CACHE, 2 * HD), BF16),
            pltpu.VMEM((KEYS, 2 * SPAN), F32),
            pltpu.VMEM((2, ZN, 2, rows, HD), BF16),
            pltpu.VMEM((2, ZN, 2, rows, HD), BF16),
            pltpu.VMEM((2, ZN, 8, SPAN), F32),
            pltpu.VMEM((2, ZN, 2, 8, SPAN), F32),
            pltpu.VMEM((rows, 4 * HD), BF16),
            pltpu.VMEM((CHIPS, ROWS, D), BF16),
            pltpu.VMEM((CHIPS, ROWS, D), BF16),
            dma((11,)),
            dma((7,)),
            dma((16,)),
            dma((8,)),
            dma((6,)),
            dma((8,)),
            dma((6,)),
            dma((8,)),
            dma((12,)),
            dma((16,)),
            dma(()),
            dma(()),
            dma((14,)),
            dma((16,)),
            dma((14,)),
            dma((16,)),
            dma((7 * PARTS,)),
            dma((8 * PARTS,)),
        ],
        compiler_params=pltpu.CompilerParams(
            collective_id=0, has_side_effects=True, vmem_limit_bytes=60 * 1024 * 1024
        ),
        name="attention_step",
    )(latents, jnp.transpose(modulation, (1, 0, 2)), w_query, w_key, w_value, w_out, cache_k, cache_v, level_index, rotation, cached_tokens)


def solution(mesh):
    placed = (
        P(("span", "tensor"), None),
        P(),
        P(None, "tensor"),
        P(None, "tensor"),
        P(None, "tensor"),
        P("tensor", None),
        P("span", "tensor"),
        P("span", "tensor"),
        P("span"),
        P(),
        P(),
    )
    return jax.shard_map(
        body, mesh=mesh, in_specs=placed, out_specs=P(("span", "tensor"), None), check_vma=False
    )
```

```python
import functools

import jax
import jax.numpy as jnp
from jax import lax
from jax.experimental import pallas as pl
from jax.experimental.pallas import tpu as pltpu
from jax.sharding import PartitionSpec as P

HD = 128
EPSILON = 1e-06
NEG = -1e30
MESH = pl.DeviceIdType.MESH
F32 = jnp.float32
BF16 = jnp.bfloat16
SCALE2 = HD**-0.5 * 1.4426950408889634

D = 5120
HALF = D // 2
XN, ZN, YN = 4, 4, 4
CHIPS = 8
ROWS = 8
CACHE = 256
SPAN = 128
KEYS = XN * (CACHE + SPAN)
NEAR = ((0, 1), (0, 3), (1, 1), (1, 3), (1, 0))
PARTS = 4
WIDTH = D // PARTS


def kernel(
    latents, modulation, w_query, w_key, w_value, w_out, cache_k, cache_v, level_index, rotation, cached_tokens,
    out_ref,
    level_s, rot_s, live_s, x_buf, lhs, mod, scale_rows, shift_rows, w_in, w_o, ck, cv, nk, nv, qb, slot_bias, span_bias, v_raw, scores, probs,
    o_send, o_recv, s_send, s_recv, att, p_send, p_recv, p_sum, hop_recv,
    load_sem, lat_send, lat_recv, far_send, far_recv, fwd_send, ck_send, ck_recv, q_send, q_recv, kv_send, kv_recv,
    wo_send, wo_recv, ot_send, ot_recv, st_send, st_recv, hop_send_sem, hop_recv_sem, dir_send, dir_recv,
    sum_send, sum_recv, mate_send, mate_recv,
):
    span = lax.axis_index("span")
    tensor = lax.axis_index("tensor")
    x = span // ZN
    zh = span % ZN
    zl = tensor // 8
    y = (tensor // 2) % YN
    core = tensor % 2
    chip = zl * YN + y
    other = 1 - core

    def chip_at(dl, dy):
        return ((zl + dl) % 2) * YN + (y + dy) % YN

    def chip_device(dl, dy, c):
        return (span, chip_at(dl, dy) * 2 + c)

    sibling = (span, chip * 2 + other)

    def x_device(dx):
        return (((x + dx) % XN) * ZN + zh, tensor)

    def z_device(dz, c):
        return (x * ZN + (zh + dz) % ZN, chip * 2 + c)

    def remote(src, dst, send, recv, device):
        return pltpu.make_async_remote_copy(
            src_ref=src, dst_ref=dst, send_sem=send, recv_sem=recv, device_id=device, device_id_type=MESH
        )

    scalars = [
        pltpu.make_async_copy(level_index, level_s, load_sem.at[8]),
        pltpu.make_async_copy(rotation, rot_s, load_sem.at[9]),
        pltpu.make_async_copy(cached_tokens, live_s, load_sem.at[10]),
    ]
    loads = [
        pltpu.make_async_copy(latents, x_buf.at[tensor], load_sem.at[0]),
        pltpu.make_async_copy(cache_k, ck.at[x], load_sem.at[1]),
        pltpu.make_async_copy(cache_v, v_raw, load_sem.at[2]),
        pltpu.make_async_copy(modulation, mod, load_sem.at[3]),
        pltpu.make_async_copy(w_query, w_in.at[0], load_sem.at[4]),
        pltpu.make_async_copy(w_key, w_in.at[1], load_sem.at[5]),
        pltpu.make_async_copy(w_value, w_in.at[2], load_sem.at[6]),
        pltpu.make_async_copy(w_out, w_o.at[core], load_sem.at[7]),
    ]
    for copy in loads[:1] + scalars + loads[1:]:
        copy.start()

    barrier = pltpu.get_barrier_semaphore()
    peers = [sibling]
    peers += [chip_device(dl, dy, core) for dl, dy in NEAR]
    peers += [x_device(dx) for dx in (1, 2, 3)]
    peers += [z_device(dz, c) for dz in (1, 2, 3) for c in (0, 1)]
    for device in peers:
        pl.semaphore_signal(barrier, inc=1, device_id=device, device_id_type=MESH)

    for copy in scalars:
        copy.wait()
    live = live_s[0]
    level = level_s[0]
    slot = lax.broadcasted_iota(jnp.int32, (CACHE, SPAN), 0)
    for xk in range(XN):
        base = (xk * ZN + zh) * CACHE
        slot_bias[xk * CACHE : (xk + 1) * CACHE] = jnp.where(slot + base < live, 0.0, NEG)
    for zq in range(ZN):
        order_q = rot_s[x * ZN + zq]
        for xk in range(XN):
            seen = jnp.where(rot_s[xk * ZN + zh] <= order_q, 0.0, NEG)
            span_bias[zq, xk] = jnp.full((ROWS, SPAN), seen, F32)

    loads[0].wait()
    pl.semaphore_wait(barrier, len(peers))

    waits = []

    def send(src, dst, send_sem, recv_sem, device):
        copy = remote(src, dst, send_sem, recv_sem, device)
        copy.start()
        waits.append(copy)

    own_rows = x_buf.at[tensor]
    for k, (dl, dy) in enumerate(NEAR):
        send(own_rows, own_rows, lat_send.at[k], lat_recv.at[tensor], chip_device(dl, dy, core))
    send(own_rows, own_rows, fwd_send.at[7], lat_recv.at[tensor], sibling)

    loads[1].wait()
    loads[2].wait()
    cv[x] = v_raw[...].T
    for k, dx in enumerate((1, 3, 2)):
        send(ck.at[x], ck.at[x], ck_send.at[2 * k], ck_recv.at[2 * x], x_device(dx))
        send(cv.at[x], cv.at[x], ck_send.at[2 * k + 1], ck_recv.at[2 * x + 1], x_device(dx))

    loads[3].wait()
    shift_rows[...] = jnp.broadcast_to(mod[0, pl.ds(level, 1), :], (ROWS, D))
    scale_rows[...] = jnp.broadcast_to(1.0 + mod[1, pl.ds(level, 1), :], (ROWS, D))

    def arrived(index):
        remote(x_buf.at[index], x_buf.at[index], lat_send.at[0], lat_recv.at[index], sibling).wait_recv()

    def normalised(index):
        row_data = x_buf[index].astype(F32)
        mean = jnp.sum(row_data, axis=1, keepdims=True) * (1.0 / D)
        centred = row_data - mean
        var = jnp.sum(centred * centred, axis=1, keepdims=True) * (1.0 / D)
        return centred * lax.rsqrt(var + EPSILON) * scale_rows[...] + shift_rows[...]

    def normalise_pair(first_chip, c):
        rows = jnp.concatenate(
            [normalised(first_chip * 2 + c), normalised((first_chip + 1) * 2 + c)], axis=0
        )
        start = pl.multiple_of(c * (CHIPS * ROWS) + first_chip * ROWS, 16)
        lhs[pl.ds(start, 16), :] = rows.astype(BF16)

    def group_chip(dl, dp):
        return ((zl + dl) % 2) * YN + ((y // 2 + dp) % 2) * 2

    def sibling_pair(first):
        arrived(first * 2 + other)
        arrived((first + 1) * 2 + other)
        normalise_pair(first, other)

    def pass_on(index, k):
        piece = x_buf.at[index]
        send(piece, piece, fwd_send.at[k], lat_recv.at[index], sibling)

    for k, (dl, dy) in enumerate(NEAR):
        index = chip_at(dl, dy) * 2 + core
        arrived(index)
        if dy:
            side = 0 if dy == 3 else 1
            piece = x_buf.at[index, :, side * HALF : (side + 1) * HALF]
            send(piece, piece, far_send.at[2 * dl + side], far_recv.at[2 * dl + side], chip_device(0, 4 - dy, core))
        pass_on(index, k)
    near = [group_chip(dl, 0) for dl in range(2)]
    far = [group_chip(dl, 1) for dl in range(2)]
    for first in near:
        normalise_pair(first, core)
    for first in near:
        sibling_pair(first)
    for dl, first in enumerate(far):
        index = chip_at(dl, 2) * 2 + core
        for side in range(2):
            piece = x_buf.at[index, :, side * HALF : (side + 1) * HALF]
            remote(piece, piece, far_send.at[0], far_recv.at[2 * dl + side], sibling).wait_recv()
        pass_on(index, 5 + dl)
        normalise_pair(first, core)
    for first in far:
        sibling_pair(first)

    always = jnp.full((1, 1), span, jnp.int32) >= 0

    def project(which):
        sums = [None, None]
        for n in range(D // 256):
            depth = slice(n // 2 * 256 + n % 2 * HALF, (n // 2 + 1) * 256 + n % 2 * HALF)
            part = jnp.dot(lhs[:, depth], w_in[which, depth], preferred_element_type=F32)
            sums[n % 2] = part if sums[n % 2] is None else sums[n % 2] + part
        return (sums[0] + jnp.where(always, sums[1], 0.0)).astype(BF16)

    loads[4].wait()
    queries = project(0)
    for h in range(2):
        qb[h, zh] = queries[:, h * HD : (h + 1) * HD]
    for h in range(2):
        for k, dz in enumerate((2, 1, 3)):
            send(qb.at[h, zh], qb.at[h, zh], q_send.at[3 * h + k], q_recv.at[4 * h + zh], z_device(dz, core))

    def send_rows(buf, v, h):
        for k, dx in enumerate((1, 3, 2)):
            send(
                buf.at[h, x], buf.at[h, x], kv_send.at[3 * (2 * v + h) + k], kv_recv.at[4 * (2 * v + h) + x], x_device(dx)
            )

    loads[5].wait()
    keys = project(1)
    for h in range(2):
        nk[h, x] = keys[:, h * HD : (h + 1) * HD]
    send_rows(nk, 0, 0)
    loads[6].wait()
    values = project(2)
    for h in range(2):
        nv[h, x] = values[:, h * HD : (h + 1) * HD].T
    send_rows(nv, 1, 0)
    send_rows(nk, 0, 1)
    send_rows(nv, 1, 1)
    loads[7].wait()
    send(w_o.at[core], w_o.at[core], wo_send, wo_recv, sibling)

    def key_chunk(h, j):
        if j < XN:
            return ck[j, :, h * HD : (h + 1) * HD]
        j -= XN
        return nk[h, 2 * j : 2 * j + 2].reshape(2 * SPAN, HD)

    def value_chunk(h, j):
        if j < XN:
            return cv[j, h * HD : (h + 1) * HD, :]
        j -= XN
        return jnp.concatenate([nv[h, 2 * j], nv[h, 2 * j + 1]], axis=1)

    def mask_chunk(zqs, j):
        if j < XN:
            tile = slot_bias[j * CACHE : (j + 1) * CACHE]
            return jnp.concatenate([tile] * len(zqs), axis=1)
        j -= XN
        rows = []
        for xk in (2 * j, 2 * j + 1):
            tile = jnp.concatenate([span_bias[zq, xk] for zq in zqs], axis=1)
            rows.append(jnp.broadcast_to(tile[None], (SPAN // ROWS, *tile.shape)).reshape(SPAN, -1))
        return jnp.concatenate(rows, axis=0)

    chunks = KEYS // 256

    def attend(h, zqs):
        width = len(zqs) * SPAN
        q = jnp.concatenate([qb[h, zq] for zq in zqs], axis=0)
        top = None
        for j in range(chunks):
            s = lax.dot_general(key_chunk(h, j), q, (((1,), (1,)), ((), ())), preferred_element_type=F32)
            s = s + mask_chunk(zqs, j)
            scores[j * 256 : (j + 1) * 256] = s
            best = jnp.max(s.reshape(256 // ROWS, ROWS, width), axis=0)
            top = best if top is None else jnp.maximum(top, best)
        top = jnp.max(top, axis=0, keepdims=True)
        peak = jnp.broadcast_to(top, (ROWS, width))
        step = 128

        def weigh(n, total):
            rows = pl.ds(pl.multiple_of(n * step, step), step)
            p = jnp.exp2((scores[rows].reshape(step // ROWS, ROWS, width) - peak) * SCALE2)
            probs[rows] = p.reshape(step, width).astype(BF16)
            return total + jnp.sum(p, axis=0)

        total = lax.fori_loop(0, KEYS // step, weigh, jnp.zeros((ROWS, width), F32))
        sums = [None, None]
        for j in range(chunks):
            part = jnp.dot(value_chunk(h, j), probs[j * 256 : (j + 1) * 256], preferred_element_type=F32)
            sums[j % 2] = part if sums[j % 2] is None else sums[j % 2] + part
        acc = sums[0] + jnp.where(always, sums[1], 0.0)
        total = jnp.sum(total, axis=0, keepdims=True)
        lse = top * SCALE2 + jnp.log2(total)
        acc = acc / total
        out = []
        for n in range(len(zqs)):
            cols = slice(n * SPAN, (n + 1) * SPAN)
            out.append((acc[:, cols].T.astype(BF16), lse[:, cols]))
        return out

    for h in range(2):
        for dx in (1, 3, 2):
            xk = (x + dx) % XN
            if h == 0:
                remote(ck.at[xk], ck.at[xk], ck_send.at[0], ck_recv.at[2 * xk], sibling).wait_recv()
                remote(cv.at[xk], cv.at[xk], ck_send.at[0], ck_recv.at[2 * xk + 1], sibling).wait_recv()
            remote(nk.at[h, xk], nk.at[h, xk], kv_send.at[0], kv_recv.at[4 * h + xk], sibling).wait_recv()
            remote(nv.at[h, xk], nv.at[h, xk], kv_send.at[0], kv_recv.at[8 + 4 * h + xk], sibling).wait_recv()
        results = []
        for k, dz in enumerate((1, 3, 2, 0)):
            zq = (zh + dz) % ZN
            if k % 2 == 0:
                pair = [1, 3] if k == 0 else [2, 0]
                zqs = [(zh + d) % ZN for d in pair]
                for d, z in zip(pair, zqs):
                    if d:
                        remote(qb.at[h, z], qb.at[h, z], q_send.at[0], q_recv.at[4 * h + z], sibling).wait_recv()
                results += attend(h, zqs)
            part, stat = results[k]
            rows = CHIPS * ROWS
            s_send[h, zq] = stat
            o_send[h, zq, 0] = part[:rows]
            o_send[h, zq, 1] = part[rows:]
            for c in range(2):
                if dz:
                    n = 6 * h + 2 * k + c
                    slot = 8 * h + 2 * zh
                    device = z_device(dz, c)
                    send(o_send.at[h, zq, c], o_recv.at[h, zh, core], ot_send.at[n], ot_recv.at[slot + core], device)
                    send(s_send.at[h, zq], s_recv.at[h, zh, core], st_send.at[n], st_recv.at[slot + core], device)
            if dz == 0:
                send(
                    o_send.at[h, zq, other], o_recv.at[h, zh, core], ot_send.at[12 + h],
                    ot_recv.at[8 * h + 2 * zh + core], sibling,
                )
                send(
                    s_send.at[h, zq], s_recv.at[h, zh, core], st_send.at[12 + h],
                    st_recv.at[8 * h + 2 * zh + core], sibling,
                )
                o_recv[h, zh, core] = o_send[h, zh, core]
                s_recv[h, zh, core] = s_send[h, zh]

    rows = CHIPS * ROWS
    mine = lax.broadcasted_iota(jnp.int32, (rows, SPAN), 1) == core * rows + lax.broadcasted_iota(
        jnp.int32, (rows, SPAN), 0
    )
    for h in range(2):
        for dz in (0, 1, 3, 2):
            zs = (zh + dz) % ZN
            for dc in range(2):
                cs = (core + dc) % 2
                if dz or dc:
                    slot = 8 * h + 2 * zs + cs
                    remote(o_recv.at[h, zs, cs], o_recv.at[h, zs, cs], ot_send.at[0], ot_recv.at[slot], sibling).wait_recv()
                    remote(s_recv.at[h, zs, cs], s_recv.at[h, zs, cs], st_send.at[0], st_recv.at[slot], sibling).wait_recv()
        for cs in range(2):
            lses = [
                jnp.sum(jnp.where(mine, s_recv[h, zs, cs], 0.0), axis=1, keepdims=True) for zs in range(ZN)
            ]
            best = jnp.maximum(jnp.maximum(lses[0], lses[1]), jnp.maximum(lses[2], lses[3]))
            shares = [jnp.exp2(value - best) for value in lses]
            whole = shares[0] + shares[1] + shares[2] + shares[3]
            summed = sum(shares[zs] * o_recv[h, zs, cs].astype(F32) for zs in range(ZN))
            att[:, (2 * cs + h) * HD : (2 * cs + h + 1) * HD] = (summed / whole).astype(BF16)

    remote(w_o.at[other], w_o.at[other], wo_send, wo_recv, sibling).wait_recv()
    def halves(part, side):
        return pl.ds(part * WIDTH + side * (WIDTH // 2), WIDTH // 2)

    for part in range(PARTS):
        cols = pl.ds(part * WIDTH, WIDTH)
        for n in range(WIDTH // 256):
            sub = pl.ds(part * WIDTH + n * 256, 256)
            value = jnp.dot(att[:, : 2 * HD], w_o[0, :, sub], preferred_element_type=F32) + jnp.dot(
                att[:, 2 * HD :], w_o[1, :, sub], preferred_element_type=F32
            )
            p_send[:, :, sub] = value.reshape(CHIPS, ROWS, 256).astype(BF16)
        for dl in range(2):
            for side in range(2):
                n = 4 * part + 2 * dl + side
                send(
                    p_send.at[chip_at(dl, 2), :, halves(part, side)], hop_recv.at[n],
                    hop_send_sem.at[n], hop_recv_sem.at[n], chip_device(0, 1 if side == 0 else 3, core),
                )
        for dl in range(2):
            for side in range(2):
                half = halves(part, 1 - side)
                dy = 1 if side == 0 else 3
                n = 4 * part + 2 * dl + side
                send(
                    p_send.at[chip_at(dl, dy), :, half], p_recv.at[chip, :, half],
                    dir_send.at[n], dir_recv.at[n], chip_device(dl, dy, core),
                )
        send(
            p_send.at[chip_at(1, 0), :, cols], p_recv.at[chip, :, cols], mate_send.at[part], mate_recv.at[part],
            chip_device(1, 0, core),
        )

    for part in range(PARTS):
        for dl in range(2):
            for side in range(2):
                half = halves(part, side)
                n = 4 * part + 2 * dl + side
                held = hop_recv.at[n]
                remote(held, held, hop_send_sem.at[0], hop_recv_sem.at[n], sibling).wait_recv()
                dy = 1 if side == 0 else 3
                index = chip_at(dl, dy)
                added = p_send[index, :, half].astype(F32) + held[...].astype(F32)
                p_sum[n] = added.astype(BF16)
                send(
                    p_sum.at[n], p_recv.at[chip, :, half], sum_send.at[n], sum_recv.at[n], chip_device(dl, dy, core),
                )

    gate = mod[2, pl.ds(level, 1), :]
    for part in range(PARTS):
        cols = pl.ds(part * WIDTH, WIDTH)
        total = p_send[chip, :, cols].astype(F32)
        mate = p_recv.at[chip_at(1, 0), :, cols]
        remote(mate, mate, mate_send.at[0], mate_recv.at[part], sibling).wait_recv()
        total = total + mate[...].astype(F32)
        for dl in range(2):
            for side in range(2):
                source = chip_at(dl, 3 if side == 0 else 1)
                n = 4 * part + 2 * dl + side
                late = p_recv.at[source, :, halves(part, side)]
                early = p_recv.at[source, :, halves(part, 1 - side)]
                remote(early, early, dir_send.at[0], dir_recv.at[n], sibling).wait_recv()
                remote(late, late, sum_send.at[0], sum_recv.at[n], sibling).wait_recv()
                total = total + p_recv[source, :, cols].astype(F32)
        out_ref[:, cols] = (gate[:, part * WIDTH : (part + 1) * WIDTH] * total).astype(BF16)

    for copy in waits:
        copy.wait_send()


def body(
    latents, modulation, w_query, w_key, w_value, w_out, cache_k, cache_v, level_index, rotation, cached_tokens
):
    anywhere = pl.BlockSpec(memory_space=pltpu.HBM)
    dma = pltpu.SemaphoreType.DMA
    rows = CHIPS * ROWS
    return pl.pallas_call(
        kernel,
        out_shape=jax.ShapeDtypeStruct((ROWS, D), BF16),
        in_specs=[anywhere] * 11,
        out_specs=pl.BlockSpec(memory_space=pltpu.VMEM),
        scratch_shapes=[
            pltpu.SMEM((1,), jnp.int32),
            pltpu.SMEM((16,), jnp.int32),
            pltpu.SMEM((1,), jnp.int32),
            pltpu.VMEM((16, ROWS, D), BF16),
            pltpu.VMEM((SPAN, D), BF16),
            pltpu.VMEM((3, 4, D), F32),
            pltpu.VMEM((ROWS, D), F32),
            pltpu.VMEM((ROWS, D), F32),
            pltpu.VMEM((3, D, 2 * HD), BF16),
            pltpu.VMEM((2, 2 * HD, D), BF16),
            pltpu.VMEM((XN, CACHE, 2 * HD), BF16),
            pltpu.VMEM((XN, 2 * HD, CACHE), BF16),
            pltpu.VMEM((2, XN, SPAN, HD), BF16),
            pltpu.VMEM((2, XN, HD, SPAN), BF16),
            pltpu.VMEM((2, ZN, SPAN, HD), BF16),
            pltpu.VMEM((XN * CACHE, SPAN), F32),
            pltpu.VMEM((ZN, XN, ROWS, SPAN), F32),
            pltpu.VMEM((CACHE, 2 * HD), BF16),
            pltpu.VMEM((KEYS, 2 * SPAN), F32),
            pltpu.VMEM((KEYS, 2 * SPAN), BF16),
            pltpu.VMEM((2, ZN, 2, rows, HD), BF16),
            pltpu.VMEM((2, ZN, 2, rows, HD), BF16),
            pltpu.VMEM((2, ZN, 1, SPAN), F32),
            pltpu.VMEM((2, ZN, 2, 1, SPAN), F32),
            pltpu.VMEM((rows, 4 * HD), BF16),
            pltpu.VMEM((CHIPS, ROWS, D), BF16),
            pltpu.VMEM((CHIPS, ROWS, D), BF16),
            pltpu.VMEM((4 * PARTS, ROWS, WIDTH // 2), BF16),
            pltpu.VMEM((4 * PARTS, ROWS, WIDTH // 2), BF16),
            dma((11,)),
            dma((5,)),
            dma((16,)),
            dma((4,)),
            dma((4,)),
            dma((8,)),
            dma((6,)),
            dma((8,)),
            dma((6,)),
            dma((8,)),
            dma((12,)),
            dma((16,)),
            dma(()),
            dma(()),
            dma((14,)),
            dma((16,)),
            dma((14,)),
            dma((16,)),
            dma((4 * PARTS,)),
            dma((4 * PARTS,)),
            dma((4 * PARTS,)),
            dma((4 * PARTS,)),
            dma((4 * PARTS,)),
            dma((4 * PARTS,)),
            dma((PARTS,)),
            dma((PARTS,)),
        ],
        compiler_params=pltpu.CompilerParams(
            collective_id=0, has_side_effects=True, vmem_limit_bytes=60 * 1024 * 1024
        ),
        name="attention_step",
    )(latents, jnp.transpose(modulation, (1, 0, 2)), w_query, w_key, w_value, w_out, cache_k, cache_v, level_index, rotation, cached_tokens)


def solution(mesh):
    placed = (
        P(("span", "tensor"), None),
        P(),
        P(None, "tensor"),
        P(None, "tensor"),
        P(None, "tensor"),
        P("tensor", None),
        P("span", "tensor"),
        P("span", "tensor"),
        P("span"),
        P(),
        P(),
    )
    return jax.shard_map(
        body, mesh=mesh, in_specs=placed, out_specs=P(("span", "tensor"), None), check_vma=False
    )
```

```python
import functools

import jax
import jax.numpy as jnp
from jax import lax
from jax.experimental import pallas as pl
from jax.experimental.pallas import tpu as pltpu
from jax.sharding import PartitionSpec as P

HD = 128
EPSILON = 1e-06
NEG = -1e30
MESH = pl.DeviceIdType.MESH
F32 = jnp.float32
BF16 = jnp.bfloat16
SCALE2 = HD**-0.5 * 1.4426950408889634

D = 5120
HALF = D // 2
XN, ZN, YN = 4, 4, 4
CHIPS = 8
ROWS = 8
CACHE = 256
SPAN = 128
KEYS = XN * (CACHE + SPAN)
NEAR = ((0, 1), (0, 3), (1, 1), (1, 3), (1, 0))
PLANE = 64
PARTS = 1
WIDTH = D // PARTS


def kernel(
    latents, modulation, w_query, w_key, w_value, w_out, cache_k, cache_v, level_index, rotation, cached_tokens,
    out_ref,
    level_s, rot_s, live_s, x_buf, lhs, mod, scale_rows, shift_rows, w_in, w_o, ck, cv, kv, nv, qb, slot_bias, span_bias, v_raw, scores, probs,
    o_send, o_recv, s_send, s_recv, att, p_send, p_recv, p_sum, hop_recv,
    load_sem, lat_send, lat_recv, far_send, far_recv, fwd_send, ck_send, ck_recv, q_send, q_recv, kv_send, kv_recv,
    wo_send, wo_recv, ot_send, ot_recv, st_send, st_recv, hop_send_sem, hop_recv_sem, dir_send, dir_recv,
    sum_send, sum_recv, mate_send, mate_recv,
):
    span = lax.axis_index("span")
    tensor = lax.axis_index("tensor")
    x = span // ZN
    zh = span % ZN
    zl = tensor // 8
    y = (tensor // 2) % YN
    core = tensor % 2
    chip = zl * YN + y
    other = 1 - core

    def chip_at(dl, dy):
        return ((zl + dl) % 2) * YN + (y + dy) % YN

    def chip_device(dl, dy, c):
        return (span, chip_at(dl, dy) * 2 + c)

    sibling = (span, chip * 2 + other)

    def x_device(dx):
        return (((x + dx) % XN) * ZN + zh, tensor)

    def z_device(dz, c):
        return (x * ZN + (zh + dz) % ZN, chip * 2 + c)

    def remote(src, dst, send, recv, device):
        return pltpu.make_async_remote_copy(
            src_ref=src, dst_ref=dst, send_sem=send, recv_sem=recv, device_id=device, device_id_type=MESH
        )

    scalars = [
        pltpu.make_async_copy(level_index, level_s, load_sem.at[8]),
        pltpu.make_async_copy(rotation, rot_s, load_sem.at[9]),
        pltpu.make_async_copy(cached_tokens, live_s, load_sem.at[10]),
    ]
    loads = [
        pltpu.make_async_copy(latents, x_buf.at[tensor], load_sem.at[0]),
        pltpu.make_async_copy(cache_k, ck.at[x], load_sem.at[1]),
        pltpu.make_async_copy(cache_v, v_raw, load_sem.at[2]),
        pltpu.make_async_copy(modulation, mod, load_sem.at[3]),
        pltpu.make_async_copy(w_query, w_in.at[0], load_sem.at[4]),
        pltpu.make_async_copy(w_key, w_in.at[1], load_sem.at[5]),
        pltpu.make_async_copy(w_value, w_in.at[2], load_sem.at[6]),
        pltpu.make_async_copy(w_out, w_o.at[core], load_sem.at[7]),
    ]
    for copy in loads[:1] + scalars + loads[1:]:
        copy.start()

    barrier = pltpu.get_barrier_semaphore()
    peers = [sibling]
    peers += [chip_device(dl, dy, core) for dl, dy in NEAR]
    peers += [x_device(dx) for dx in (1, 2, 3)]
    peers += [z_device(dz, c) for dz in (1, 2, 3) for c in (0, 1)]
    for device in peers:
        pl.semaphore_signal(barrier, inc=1, device_id=device, device_id_type=MESH)

    for copy in scalars:
        copy.wait()
    live = live_s[0]
    level = level_s[0]
    slot = lax.broadcasted_iota(jnp.int32, (CACHE, SPAN), 0)
    for xk in range(XN):
        base = (xk * ZN + zh) * CACHE
        slot_bias[xk * CACHE : (xk + 1) * CACHE] = jnp.where(slot + base < live, 0.0, NEG)
    for zq in range(ZN):
        order_q = rot_s[x * ZN + zq]
        for xk in range(XN):
            seen = jnp.where(rot_s[xk * ZN + zh] <= order_q, 0.0, NEG)
            span_bias[zq, xk] = jnp.full((ROWS, SPAN), seen, F32)

    loads[0].wait()
    pl.semaphore_wait(barrier, len(peers))

    waits = []

    def send(src, dst, send_sem, recv_sem, device):
        copy = remote(src, dst, send_sem, recv_sem, device)
        copy.start()
        waits.append(copy)

    own_rows = x_buf.at[tensor]
    for k, (dl, dy) in enumerate(NEAR):
        send(own_rows, own_rows, lat_send.at[k], lat_recv.at[tensor], chip_device(dl, dy, core))
    send(own_rows, own_rows, fwd_send.at[7], lat_recv.at[tensor], sibling)

    loads[1].wait()
    loads[2].wait()
    cv[x] = v_raw[...].T
    for k, dx in enumerate((1, 3, 2)):
        send(ck.at[x], ck.at[x], ck_send.at[2 * k], ck_recv.at[2 * x], x_device(dx))
        send(cv.at[x], cv.at[x], ck_send.at[2 * k + 1], ck_recv.at[2 * x + 1], x_device(dx))

    loads[3].wait()
    shift_rows[...] = jnp.broadcast_to(mod[0, pl.ds(level, 1), :], (ROWS, D))
    scale_rows[...] = jnp.broadcast_to(1.0 + mod[1, pl.ds(level, 1), :], (ROWS, D))

    def arrived(index):
        remote(x_buf.at[index], x_buf.at[index], lat_send.at[0], lat_recv.at[index], sibling).wait_recv()

    def normalised(index):
        row_data = x_buf[index].astype(F32)
        mean = jnp.sum(row_data, axis=1, keepdims=True) * (1.0 / D)
        centred = row_data - mean
        var = jnp.sum(centred * centred, axis=1, keepdims=True) * (1.0 / D)
        return centred * lax.rsqrt(var + EPSILON) * scale_rows[...] + shift_rows[...]

    def normalise_pair(first_chip, c):
        rows = jnp.concatenate(
            [normalised(first_chip * 2 + c), normalised((first_chip + 1) * 2 + c)], axis=0
        )
        start = pl.multiple_of((first_chip // YN) * PLANE + c * (PLANE // 2) + (first_chip % YN) * ROWS, 16)
        lhs[pl.ds(start, 16), :] = rows.astype(BF16)

    def group_chip(dl, dp):
        return ((zl + dl) % 2) * YN + ((y // 2 + dp) % 2) * 2

    def sibling_pair(first):
        arrived(first * 2 + other)
        arrived((first + 1) * 2 + other)
        normalise_pair(first, other)

    def pass_on(index, k):
        piece = x_buf.at[index]
        send(piece, piece, fwd_send.at[k], lat_recv.at[index], sibling)

    for k, (dl, dy) in enumerate(NEAR):
        index = chip_at(dl, dy) * 2 + core
        arrived(index)
        if dy:
            side = 0 if dy == 3 else 1
            piece = x_buf.at[index, :, side * HALF : (side + 1) * HALF]
            send(piece, piece, far_send.at[2 * dl + side], far_recv.at[2 * dl + side], chip_device(0, 4 - dy, core))
        pass_on(index, k)
    always = jnp.full((1, 1), span, jnp.int32) >= 0

    def project(which, plane):
        rows = pl.ds(pl.multiple_of(plane * PLANE, PLANE), PLANE)
        sums = [None, None]
        for n in range(D // 256):
            depth = slice(n // 2 * 256 + n % 2 * HALF, (n // 2 + 1) * 256 + n % 2 * HALF)
            part = jnp.dot(lhs[rows, depth], w_in[which, depth], preferred_element_type=F32)
            sums[n % 2] = part if sums[n % 2] is None else sums[n % 2] + part
        return (sums[0] + jnp.where(always, sums[1], 0.0)).astype(BF16)

    def far_rows(dl):
        index = chip_at(dl, 2) * 2 + core
        for side in range(2):
            piece = x_buf.at[index, :, side * HALF : (side + 1) * HALF]
            remote(piece, piece, far_send.at[0], far_recv.at[2 * dl + side], sibling).wait_recv()
        pass_on(index, 5 + dl)

    for dl in range(2):
        plane = (zl + dl) % 2
        near, far = group_chip(dl, 0), group_chip(dl, 1)
        normalise_pair(near, core)
        if dl == 0:
            far_rows(0)
        sibling_pair(near)
        if dl == 1:
            far_rows(1)
        normalise_pair(far, core)
        sibling_pair(far)
        if dl == 0:
            loads[4].wait()
        queries = project(0, plane)
        for h in range(2):
            qb[zh, plane, h] = queries[:, h * HD : (h + 1) * HD]
        if dl == 0:
            for k, dz in enumerate((2, 1, 3)):
                rows = qb.at[zh, plane]
                send(rows, rows, q_send.at[k], q_recv.at[zh], z_device(dz, core))
            loads[5].wait()
            loads[6].wait()
        else:
            for h in range(2):
                for k, dz in enumerate((2, 1, 3)):
                    rows = qb.at[zh, plane, h]
                    send(rows, rows, q_send.at[3 + 3 * h + k], q_recv.at[ZN + ZN * h + zh], z_device(dz, core))
        for v in range(2):
            value = project(1 + v, plane)
            for h in range(2):
                kv[x, plane, h, v] = value[:, h * HD : (h + 1) * HD]
        if dl == 0:
            for k, dx in enumerate((2, 1, 3)):
                rows = kv.at[x, plane]
                send(rows, rows, kv_send.at[k], kv_recv.at[x], x_device(dx))
        else:
            for h in range(2):
                for k, dx in enumerate((2, 1, 3)):
                    rows = kv.at[x, plane, h]
                    send(rows, rows, kv_send.at[3 + 3 * h + k], kv_recv.at[XN + XN * h + x], x_device(dx))
    loads[7].wait()
    send(w_o.at[core], w_o.at[core], wo_send, wo_recv, sibling)

    def key_chunk(h, j):
        if j < XN:
            return ck[j, :, h * HD : (h + 1) * HD]
        j -= XN
        return jnp.concatenate([kv[xk, :, h, 0].reshape(SPAN, HD) for xk in (2 * j, 2 * j + 1)], axis=0)

    def value_chunk(h, j):
        if j < XN:
            return cv[j, h * HD : (h + 1) * HD, :]
        j -= XN
        return jnp.concatenate([nv[2 * j], nv[2 * j + 1]], axis=1)

    def mask_chunk(zqs, j):
        if j < XN:
            tile = slot_bias[j * CACHE : (j + 1) * CACHE]
            return jnp.concatenate([tile] * len(zqs), axis=1)
        j -= XN
        rows = []
        for xk in (2 * j, 2 * j + 1):
            tile = jnp.concatenate([span_bias[zq, xk] for zq in zqs], axis=1)
            rows.append(jnp.broadcast_to(tile[None], (SPAN // ROWS, *tile.shape)).reshape(SPAN, -1))
        return jnp.concatenate(rows, axis=0)

    chunks = KEYS // 256

    def attend(h, zqs):
        width = len(zqs) * SPAN
        q = jnp.concatenate([qb[zq, :, h].reshape(SPAN, HD) for zq in zqs], axis=0)
        top = None
        for j in range(chunks):
            s = lax.dot_general(key_chunk(h, j), q, (((1,), (1,)), ((), ())), preferred_element_type=F32)
            s = s + mask_chunk(zqs, j)
            scores[j * 256 : (j + 1) * 256] = s
            best = jnp.max(s.reshape(256 // ROWS, ROWS, width), axis=0)
            top = best if top is None else jnp.maximum(top, best)
        top = jnp.max(top, axis=0, keepdims=True)
        peak = jnp.broadcast_to(top, (ROWS, width))
        step = 128

        def weigh(n, total):
            rows = pl.ds(pl.multiple_of(n * step, step), step)
            p = jnp.exp2((scores[rows].reshape(step // ROWS, ROWS, width) - peak) * SCALE2)
            probs[rows] = p.reshape(step, width).astype(BF16)
            return total + jnp.sum(p, axis=0)

        total = lax.fori_loop(0, KEYS // step, weigh, jnp.zeros((ROWS, width), F32))
        sums = [None, None]
        for j in range(chunks):
            part = jnp.dot(value_chunk(h, j), probs[j * 256 : (j + 1) * 256], preferred_element_type=F32)
            sums[j % 2] = part if sums[j % 2] is None else sums[j % 2] + part
        acc = sums[0] + jnp.where(always, sums[1], 0.0)
        total = jnp.sum(total, axis=0, keepdims=True)
        lse = top * SCALE2 + jnp.log2(total)
        acc = acc / total
        out = []
        for n in range(len(zqs)):
            cols = slice(n * SPAN, (n + 1) * SPAN)
            out.append((acc[:, cols].T.astype(BF16), lse[:, cols]))
        return out

    for h in range(2):
        for dx in (1, 3, 2):
            xk = (x + dx) % XN
            if h == 0:
                remote(ck.at[xk], ck.at[xk], ck_send.at[0], ck_recv.at[2 * xk], sibling).wait_recv()
                remote(cv.at[xk], cv.at[xk], ck_send.at[0], ck_recv.at[2 * xk + 1], sibling).wait_recv()
                rows = kv.at[xk, zl]
                remote(rows, rows, kv_send.at[0], kv_recv.at[xk], sibling).wait_recv()
            rows = kv.at[xk, 1 - zl, h]
            remote(rows, rows, kv_send.at[0], kv_recv.at[XN + XN * h + xk], sibling).wait_recv()
        for xk in range(XN):
            nv[xk] = kv[xk, :, h, 1].reshape(SPAN, HD).T
        results = []
        for k, dz in enumerate((2, 1, 3, 0)):
            zq = (zh + dz) % ZN
            if k % 2 == 0:
                pair = [2, 1] if k == 0 else [3, 0]
                zqs = [(zh + d) % ZN for d in pair]
                for d, z in zip(pair, zqs):
                    if d:
                        if h == 0:
                            rows = qb.at[z, zl]
                            remote(rows, rows, q_send.at[0], q_recv.at[z], sibling).wait_recv()
                        rows = qb.at[z, 1 - zl, h]
                        remote(rows, rows, q_send.at[0], q_recv.at[ZN + ZN * h + z], sibling).wait_recv()
                results += attend(h, zqs)
            part, stat = results[k]
            s_send[h, zq] = stat
            for c in range(2):
                quarter = PLANE // 2
                for plane in range(2):
                    start = plane * PLANE + c * quarter
                    o_send[h, zq, c, plane * quarter : (plane + 1) * quarter] = part[start : start + quarter]
            for c in range(2):
                if dz:
                    n = 6 * h + 2 * k + c
                    slot = 8 * h + 2 * zh
                    device = z_device(dz, c)
                    send(o_send.at[h, zq, c], o_recv.at[h, zh, core], ot_send.at[n], ot_recv.at[slot + core], device)
                    send(s_send.at[h, zq], s_recv.at[h, zh, core], st_send.at[n], st_recv.at[slot + core], device)
            if dz == 0:
                send(
                    o_send.at[h, zq, other], o_recv.at[h, zh, core], ot_send.at[12 + h],
                    ot_recv.at[8 * h + 2 * zh + core], sibling,
                )
                send(
                    s_send.at[h, zq], s_recv.at[h, zh, core], st_send.at[12 + h],
                    st_recv.at[8 * h + 2 * zh + core], sibling,
                )
                o_recv[h, zh, core] = o_send[h, zh, core]
                s_recv[h, zh, core] = s_send[h, zh]

    rows = CHIPS * ROWS
    place = lax.broadcasted_iota(jnp.int32, (rows, SPAN), 0)
    place = jnp.where(place < PLANE // 2, place, place + PLANE // 2) + core * (PLANE // 2)
    mine = lax.broadcasted_iota(jnp.int32, (rows, SPAN), 1) == place
    for h in range(2):
        for dz in (0, 1, 3, 2):
            zs = (zh + dz) % ZN
            for dc in range(2):
                cs = (core + dc) % 2
                if dz or dc:
                    slot = 8 * h + 2 * zs + cs
                    remote(o_recv.at[h, zs, cs], o_recv.at[h, zs, cs], ot_send.at[0], ot_recv.at[slot], sibling).wait_recv()
                    remote(s_recv.at[h, zs, cs], s_recv.at[h, zs, cs], st_send.at[0], st_recv.at[slot], sibling).wait_recv()
        for cs in range(2):
            lses = [
                jnp.sum(jnp.where(mine, s_recv[h, zs, cs], 0.0), axis=1, keepdims=True) for zs in range(ZN)
            ]
            best = jnp.maximum(jnp.maximum(lses[0], lses[1]), jnp.maximum(lses[2], lses[3]))
            shares = [jnp.exp2(value - best) for value in lses]
            whole = shares[0] + shares[1] + shares[2] + shares[3]
            summed = sum(shares[zs] * o_recv[h, zs, cs].astype(F32) for zs in range(ZN))
            att[:, (2 * cs + h) * HD : (2 * cs + h + 1) * HD] = (summed / whole).astype(BF16)

    remote(w_o.at[other], w_o.at[other], wo_send, wo_recv, sibling).wait_recv()
    def halves(part, side):
        return pl.ds(part * WIDTH + side * (WIDTH // 2), WIDTH // 2)

    for part in range(PARTS):
        cols = pl.ds(part * WIDTH, WIDTH)
        for n in range(WIDTH // 256):
            sub = pl.ds(part * WIDTH + n * 256, 256)
            value = jnp.dot(att[:, : 2 * HD], w_o[0, :, sub], preferred_element_type=F32) + jnp.dot(
                att[:, 2 * HD :], w_o[1, :, sub], preferred_element_type=F32
            )
            p_send[:, :, sub] = value.reshape(CHIPS, ROWS, 256).astype(BF16)
        for dl in range(2):
            for side in range(2):
                n = 4 * part + 2 * dl + side
                send(
                    p_send.at[chip_at(dl, 2), :, halves(part, side)], hop_recv.at[n],
                    hop_send_sem.at[n], hop_recv_sem.at[n], chip_device(0, 1 if side == 0 else 3, core),
                )
        for dl in range(2):
            for side in range(2):
                half = halves(part, 1 - side)
                dy = 1 if side == 0 else 3
                n = 4 * part + 2 * dl + side
                send(
                    p_send.at[chip_at(dl, dy), :, half], p_recv.at[chip, :, half],
                    dir_send.at[n], dir_recv.at[n], chip_device(dl, dy, core),
                )
        send(
            p_send.at[chip_at(1, 0), :, cols], p_recv.at[chip, :, cols], mate_send.at[part], mate_recv.at[part],
            chip_device(1, 0, core),
        )

    for part in range(PARTS):
        for dl in range(2):
            for side in range(2):
                half = halves(part, side)
                n = 4 * part + 2 * dl + side
                held = hop_recv.at[n]
                remote(held, held, hop_send_sem.at[0], hop_recv_sem.at[n], sibling).wait_recv()
                dy = 1 if side == 0 else 3
                index = chip_at(dl, dy)
                added = p_send[index, :, half].astype(F32) + held[...].astype(F32)
                p_sum[n] = added.astype(BF16)
                send(
                    p_sum.at[n], p_recv.at[chip, :, half], sum_send.at[n], sum_recv.at[n], chip_device(dl, dy, core),
                )

    gate = mod[2, pl.ds(level, 1), :]
    for part in range(PARTS):
        cols = pl.ds(part * WIDTH, WIDTH)
        total = p_send[chip, :, cols].astype(F32)
        mate = p_recv.at[chip_at(1, 0), :, cols]
        remote(mate, mate, mate_send.at[0], mate_recv.at[part], sibling).wait_recv()
        total = total + mate[...].astype(F32)
        for dl in range(2):
            for side in range(2):
                source = chip_at(dl, 3 if side == 0 else 1)
                n = 4 * part + 2 * dl + side
                late = p_recv.at[source, :, halves(part, side)]
                early = p_recv.at[source, :, halves(part, 1 - side)]
                remote(early, early, dir_send.at[0], dir_recv.at[n], sibling).wait_recv()
                remote(late, late, sum_send.at[0], sum_recv.at[n], sibling).wait_recv()
                total = total + p_recv[source, :, cols].astype(F32)
        out_ref[:, cols] = (gate[:, part * WIDTH : (part + 1) * WIDTH] * total).astype(BF16)

    for copy in waits:
        copy.wait_send()


def body(
    latents, modulation, w_query, w_key, w_value, w_out, cache_k, cache_v, level_index, rotation, cached_tokens
):
    anywhere = pl.BlockSpec(memory_space=pltpu.HBM)
    dma = pltpu.SemaphoreType.DMA
    rows = CHIPS * ROWS
    return pl.pallas_call(
        kernel,
        out_shape=jax.ShapeDtypeStruct((ROWS, D), BF16),
        in_specs=[anywhere] * 11,
        out_specs=pl.BlockSpec(memory_space=pltpu.VMEM),
        scratch_shapes=[
            pltpu.SMEM((1,), jnp.int32),
            pltpu.SMEM((16,), jnp.int32),
            pltpu.SMEM((1,), jnp.int32),
            pltpu.VMEM((16, ROWS, D), BF16),
            pltpu.VMEM((SPAN, D), BF16),
            pltpu.VMEM((3, 4, D), F32),
            pltpu.VMEM((ROWS, D), F32),
            pltpu.VMEM((ROWS, D), F32),
            pltpu.VMEM((3, D, 2 * HD), BF16),
            pltpu.VMEM((2, 2 * HD, D), BF16),
            pltpu.VMEM((XN, CACHE, 2 * HD), BF16),
            pltpu.VMEM((XN, 2 * HD, CACHE), BF16),
            pltpu.VMEM((XN, 2, 2, 2, PLANE, HD), BF16),
            pltpu.VMEM((XN, HD, SPAN), BF16),
            pltpu.VMEM((ZN, 2, 2, PLANE, HD), BF16),
            pltpu.VMEM((XN * CACHE, SPAN), F32),
            pltpu.VMEM((ZN, XN, ROWS, SPAN), F32),
            pltpu.VMEM((CACHE, 2 * HD), BF16),
            pltpu.VMEM((KEYS, 2 * SPAN), F32),
            pltpu.VMEM((KEYS, 2 * SPAN), BF16),
            pltpu.VMEM((2, ZN, 2, rows, HD), BF16),
            pltpu.VMEM((2, ZN, 2, rows, HD), BF16),
            pltpu.VMEM((2, ZN, 1, SPAN), F32),
            pltpu.VMEM((2, ZN, 2, 1, SPAN), F32),
            pltpu.VMEM((rows, 4 * HD), BF16),
            pltpu.VMEM((CHIPS, ROWS, D), BF16),
            pltpu.VMEM((CHIPS, ROWS, D), BF16),
            pltpu.VMEM((4 * PARTS, ROWS, WIDTH // 2), BF16),
            pltpu.VMEM((4 * PARTS, ROWS, WIDTH // 2), BF16),
            dma((11,)),
            dma((5,)),
            dma((16,)),
            dma((4,)),
            dma((4,)),
            dma((8,)),
            dma((6,)),
            dma((8,)),
            dma((9,)),
            dma((12,)),
            dma((9,)),
            dma((12,)),
            dma(()),
            dma(()),
            dma((14,)),
            dma((16,)),
            dma((14,)),
            dma((16,)),
            dma((4 * PARTS,)),
            dma((4 * PARTS,)),
            dma((4 * PARTS,)),
            dma((4 * PARTS,)),
            dma((4 * PARTS,)),
            dma((4 * PARTS,)),
            dma((PARTS,)),
            dma((PARTS,)),
        ],
        compiler_params=pltpu.CompilerParams(
            collective_id=0, has_side_effects=True, vmem_limit_bytes=60 * 1024 * 1024
        ),
        name="attention_step",
    )(latents, jnp.transpose(modulation, (1, 0, 2)), w_query, w_key, w_value, w_out, cache_k, cache_v, level_index, rotation, cached_tokens)


def solution(mesh):
    placed = (
        P(("span", "tensor"), None),
        P(),
        P(None, "tensor"),
        P(None, "tensor"),
        P(None, "tensor"),
        P("tensor", None),
        P("span", "tensor"),
        P("span", "tensor"),
        P("span"),
        P(),
        P(),
    )
    return jax.shard_map(
        body, mesh=mesh, in_specs=placed, out_specs=P(("span", "tensor"), None), check_vma=False
    )
```

```python
import functools

import jax
import jax.numpy as jnp
from jax import lax
from jax.experimental import pallas as pl
from jax.experimental.pallas import tpu as pltpu
from jax.sharding import PartitionSpec as P

HD = 128
EPSILON = 1e-06
NEG = -1e30
MESH = pl.DeviceIdType.MESH
F32 = jnp.float32
BF16 = jnp.bfloat16
SCALE2 = HD**-0.5 * 1.4426950408889634

D = 5120
HALF = D // 2
XN, ZN, YN = 4, 4, 4
CHIPS = 8
ROWS = 8
CACHE = 256
SPAN = 128
KEYS = XN * (CACHE + SPAN)
NEAR = ((0, 1), (0, 3), (1, 1), (1, 3), (1, 0))
PARTS = 2
WIDTH = D // PARTS


def kernel(
    latents, modulation, w_query, w_key, w_value, w_out, cache_k, cache_v, level_index, rotation, cached_tokens,
    out_ref,
    level_s, rot_s, live_s, x_buf, lhs, mod, scale_rows, shift_rows, w_in, w_o, ck, cv, nk, nv, qb, slot_bias, span_bias, v_raw, scores, probs,
    o_send, o_recv, s_send, s_recv, att, p_send, p_recv, p_sum, hop_recv,
    load_sem, lat_send, lat_recv, far_send, far_recv, fwd_send, ck_send, ck_recv, q_send, q_recv, kv_send, kv_recv,
    wo_send, wo_recv, ot_send, ot_recv, st_send, st_recv, hop_send_sem, hop_recv_sem, dir_send, dir_recv,
    sum_send, sum_recv, mate_send, mate_recv,
):
    span = lax.axis_index("span")
    tensor = lax.axis_index("tensor")
    x = span // ZN
    zh = span % ZN
    zl = tensor // 8
    y = (tensor // 2) % YN
    core = tensor % 2
    chip = zl * YN + y
    other = 1 - core

    def chip_at(dl, dy):
        return ((zl + dl) % 2) * YN + (y + dy) % YN

    def chip_device(dl, dy, c):
        return (span, chip_at(dl, dy) * 2 + c)

    sibling = (span, chip * 2 + other)

    def x_device(dx):
        return (((x + dx) % XN) * ZN + zh, tensor)

    def z_device(dz, c):
        return (x * ZN + (zh + dz) % ZN, chip * 2 + c)

    def remote(src, dst, send, recv, device):
        return pltpu.make_async_remote_copy(
            src_ref=src, dst_ref=dst, send_sem=send, recv_sem=recv, device_id=device, device_id_type=MESH
        )

    barrier = pltpu.get_barrier_semaphore()
    peers = [z_device(dz, c) for dz in (2, 1, 3) for c in (0, 1)]
    peers += [chip_device(dl, dy, core) for dl, dy in NEAR]
    peers += [x_device(dx) for dx in (2, 1, 3)]
    peers += [sibling]
    for device in peers:
        pl.semaphore_signal(barrier, inc=1, device_id=device, device_id_type=MESH)

    scalars = [
        pltpu.make_async_copy(level_index, level_s, load_sem.at[8]),
        pltpu.make_async_copy(rotation, rot_s, load_sem.at[9]),
        pltpu.make_async_copy(cached_tokens, live_s, load_sem.at[10]),
    ]
    loads = [
        pltpu.make_async_copy(latents, x_buf.at[tensor], load_sem.at[0]),
        pltpu.make_async_copy(cache_k, ck.at[x], load_sem.at[1]),
        pltpu.make_async_copy(cache_v, v_raw, load_sem.at[2]),
        pltpu.make_async_copy(modulation, mod, load_sem.at[3]),
        pltpu.make_async_copy(w_query, w_in.at[0], load_sem.at[4]),
        pltpu.make_async_copy(w_key, w_in.at[1], load_sem.at[5]),
        pltpu.make_async_copy(w_value, w_in.at[2], load_sem.at[6]),
        pltpu.make_async_copy(w_out, w_o.at[core], load_sem.at[7]),
    ]
    for copy in loads[:1] + scalars + loads[1:]:
        copy.start()

    for copy in scalars:
        copy.wait()
    live = live_s[0]
    level = level_s[0]
    slot = lax.broadcasted_iota(jnp.int32, (CACHE, SPAN), 0)
    for xk in range(XN):
        base = (xk * ZN + zh) * CACHE
        slot_bias[xk * CACHE : (xk + 1) * CACHE] = jnp.where(slot + base < live, 0.0, NEG)
    for zq in range(ZN):
        order_q = rot_s[x * ZN + zq]
        for xk in range(XN):
            seen = jnp.where(rot_s[xk * ZN + zh] <= order_q, 0.0, NEG)
            span_bias[zq, xk] = jnp.full((ROWS, SPAN), seen, F32)

    loads[0].wait()
    pl.semaphore_wait(barrier, len(peers))

    waits = []

    def send(src, dst, send_sem, recv_sem, device):
        copy = remote(src, dst, send_sem, recv_sem, device)
        copy.start()
        waits.append(copy)

    own_rows = x_buf.at[tensor]
    for k, (dl, dy) in enumerate(NEAR):
        send(own_rows, own_rows, lat_send.at[k], lat_recv.at[tensor], chip_device(dl, dy, core))
    send(own_rows, own_rows, fwd_send.at[7], lat_recv.at[tensor], sibling)

    loads[1].wait()
    loads[2].wait()
    cv[x] = v_raw[...].T
    for k, dx in enumerate((1, 3, 2)):
        send(ck.at[x], ck.at[x], ck_send.at[2 * k], ck_recv.at[2 * x], x_device(dx))
        send(cv.at[x], cv.at[x], ck_send.at[2 * k + 1], ck_recv.at[2 * x + 1], x_device(dx))

    loads[3].wait()
    shift_rows[...] = jnp.broadcast_to(mod[0, pl.ds(level, 1), :], (ROWS, D))
    scale_rows[...] = jnp.broadcast_to(1.0 + mod[1, pl.ds(level, 1), :], (ROWS, D))

    def arrived(index):
        remote(x_buf.at[index], x_buf.at[index], lat_send.at[0], lat_recv.at[index], sibling).wait_recv()

    def normalised(index):
        row_data = x_buf[index].astype(F32)
        mean = jnp.sum(row_data, axis=1, keepdims=True) * (1.0 / D)
        centred = row_data - mean
        var = jnp.sum(centred * centred, axis=1, keepdims=True) * (1.0 / D)
        return centred * lax.rsqrt(var + EPSILON) * scale_rows[...] + shift_rows[...]

    def normalise_pair(first_chip, c):
        rows = jnp.concatenate(
            [normalised(first_chip * 2 + c), normalised((first_chip + 1) * 2 + c)], axis=0
        )
        start = pl.multiple_of(c * (CHIPS * ROWS) + first_chip * ROWS, 16)
        lhs[pl.ds(start, 16), :] = rows.astype(BF16)

    def group_chip(dl, dp):
        return ((zl + dl) % 2) * YN + ((y // 2 + dp) % 2) * 2

    def sibling_pair(first):
        arrived(first * 2 + other)
        arrived((first + 1) * 2 + other)
        normalise_pair(first, other)

    def pass_on(index, k):
        piece = x_buf.at[index]
        send(piece, piece, fwd_send.at[k], lat_recv.at[index], sibling)

    for k, (dl, dy) in enumerate(NEAR):
        index = chip_at(dl, dy) * 2 + core
        arrived(index)
        if dy:
            side = 0 if dy == 3 else 1
            piece = x_buf.at[index, :, side * HALF : (side + 1) * HALF]
            send(piece, piece, far_send.at[2 * dl + side], far_recv.at[2 * dl + side], chip_device(0, 4 - dy, core))
        pass_on(index, k)
    near = [group_chip(dl, 0) for dl in range(2)]
    far = [group_chip(dl, 1) for dl in range(2)]
    for first in near:
        normalise_pair(first, core)
    for first in near:
        sibling_pair(first)
    for dl, first in enumerate(far):
        index = chip_at(dl, 2) * 2 + core
        for side in range(2):
            piece = x_buf.at[index, :, side * HALF : (side + 1) * HALF]
            remote(piece, piece, far_send.at[0], far_recv.at[2 * dl + side], sibling).wait_recv()
        pass_on(index, 5 + dl)
        normalise_pair(first, core)
    for first in far:
        sibling_pair(first)

    always = jnp.full((1, 1), span, jnp.int32) >= 0

    def project(which):
        sums = [None, None]
        for n in range(D // 256):
            depth = slice(n // 2 * 256 + n % 2 * HALF, (n // 2 + 1) * 256 + n % 2 * HALF)
            part = jnp.dot(lhs[:, depth], w_in[which, depth], preferred_element_type=F32)
            sums[n % 2] = part if sums[n % 2] is None else sums[n % 2] + part
        return (sums[0] + jnp.where(always, sums[1], 0.0)).astype(BF16)

    loads[4].wait()
    queries = project(0)
    for h in range(2):
        qb[h, zh] = queries[:, h * HD : (h + 1) * HD]
    for h in range(2):
        for k, dz in enumerate((2, 1, 3)):
            send(qb.at[h, zh], qb.at[h, zh], q_send.at[3 * h + k], q_recv.at[4 * h + zh], z_device(dz, core))

    def send_rows(buf, v, h):
        for k, dx in enumerate((2, 1, 3)):
            send(
                buf.at[h, x], buf.at[h, x], kv_send.at[3 * (2 * v + h) + k], kv_recv.at[4 * (2 * v + h) + x], x_device(dx)
            )

    loads[5].wait()
    keys = project(1)
    for h in range(2):
        nk[h, x] = keys[:, h * HD : (h + 1) * HD]
    send_rows(nk, 0, 0)
    loads[6].wait()
    values = project(2)
    for h in range(2):
        nv[h, x] = values[:, h * HD : (h + 1) * HD].T
    send_rows(nv, 1, 0)
    send_rows(nk, 0, 1)
    send_rows(nv, 1, 1)
    loads[7].wait()
    send(w_o.at[core], w_o.at[core], wo_send, wo_recv, sibling)

    def key_chunk(h, j):
        if j < XN:
            return ck[j, :, h * HD : (h + 1) * HD]
        j -= XN
        return nk[h, 2 * j : 2 * j + 2].reshape(2 * SPAN, HD)

    def value_chunk(h, j):
        if j < XN:
            return cv[j, h * HD : (h + 1) * HD, :]
        j -= XN
        return jnp.concatenate([nv[h, 2 * j], nv[h, 2 * j + 1]], axis=1)

    def mask_chunk(zqs, j):
        if j < XN:
            tile = slot_bias[j * CACHE : (j + 1) * CACHE]
            return jnp.concatenate([tile] * len(zqs), axis=1)
        j -= XN
        rows = []
        for xk in (2 * j, 2 * j + 1):
            tile = jnp.concatenate([span_bias[zq, xk] for zq in zqs], axis=1)
            rows.append(jnp.broadcast_to(tile[None], (SPAN // ROWS, *tile.shape)).reshape(SPAN, -1))
        return jnp.concatenate(rows, axis=0)

    chunks = KEYS // 256

    def attend(h, zqs):
        width = len(zqs) * SPAN
        q = jnp.concatenate([qb[h, zq] for zq in zqs], axis=0)
        top = None
        for j in range(chunks):
            s = lax.dot_general(key_chunk(h, j), q, (((1,), (1,)), ((), ())), preferred_element_type=F32)
            s = s * SCALE2 + mask_chunk(zqs, j)
            scores[j * 256 : (j + 1) * 256] = s
            best = jnp.max(s.reshape(256 // ROWS, ROWS, width), axis=0)
            top = best if top is None else jnp.maximum(top, best)
        top = jnp.max(top, axis=0, keepdims=True)
        peak = jnp.broadcast_to(top, (ROWS, width))
        step = 128

        def weigh(n, total):
            rows = pl.ds(pl.multiple_of(n * step, step), step)
            p = jnp.exp2(scores[rows].reshape(step // ROWS, ROWS, width) - peak)
            probs[rows] = p.reshape(step, width).astype(BF16)
            return total + jnp.sum(p, axis=0)

        total = lax.fori_loop(0, KEYS // step, weigh, jnp.zeros((ROWS, width), F32))
        sums = [None, None]
        for j in range(chunks):
            part = jnp.dot(value_chunk(h, j), probs[j * 256 : (j + 1) * 256], preferred_element_type=F32)
            sums[j % 2] = part if sums[j % 2] is None else sums[j % 2] + part
        acc = sums[0] + jnp.where(always, sums[1], 0.0)
        total = jnp.sum(total, axis=0, keepdims=True)
        lse = top + jnp.log2(total)
        acc = acc / total
        out = []
        for n in range(len(zqs)):
            cols = slice(n * SPAN, (n + 1) * SPAN)
            out.append((acc[:, cols].T.astype(BF16), lse[:, cols]))
        return out

    for h in range(2):
        for dx in (1, 3, 2):
            xk = (x + dx) % XN
            if h == 0:
                remote(ck.at[xk], ck.at[xk], ck_send.at[0], ck_recv.at[2 * xk], sibling).wait_recv()
                remote(cv.at[xk], cv.at[xk], ck_send.at[0], ck_recv.at[2 * xk + 1], sibling).wait_recv()
            remote(nk.at[h, xk], nk.at[h, xk], kv_send.at[0], kv_recv.at[4 * h + xk], sibling).wait_recv()
            remote(nv.at[h, xk], nv.at[h, xk], kv_send.at[0], kv_recv.at[8 + 4 * h + xk], sibling).wait_recv()
        results = []
        for k, dz in enumerate((2, 1, 3, 0)):
            zq = (zh + dz) % ZN
            if k % 2 == 0:
                pair = [2, 1] if k == 0 else [3, 0]
                zqs = [(zh + d) % ZN for d in pair]
                for d, z in zip(pair, zqs):
                    if d:
                        remote(qb.at[h, z], qb.at[h, z], q_send.at[0], q_recv.at[4 * h + z], sibling).wait_recv()
                results += attend(h, zqs)
            part, stat = results[k]
            rows = CHIPS * ROWS
            s_send[h, zq] = stat
            o_send[h, zq, 0] = part[:rows]
            o_send[h, zq, 1] = part[rows:]
            for c in range(2):
                if dz:
                    n = 6 * h + 2 * k + c
                    slot = 8 * h + 2 * zh
                    device = z_device(dz, c)
                    send(o_send.at[h, zq, c], o_recv.at[h, zh, core], ot_send.at[n], ot_recv.at[slot + core], device)
                    send(s_send.at[h, zq], s_recv.at[h, zh, core], st_send.at[n], st_recv.at[slot + core], device)
            if dz == 0:
                send(
                    o_send.at[h, zq, other], o_recv.at[h, zh, core], ot_send.at[12 + h],
                    ot_recv.at[8 * h + 2 * zh + core], sibling,
                )
                send(
                    s_send.at[h, zq], s_recv.at[h, zh, core], st_send.at[12 + h],
                    st_recv.at[8 * h + 2 * zh + core], sibling,
                )
                o_recv[h, zh, core] = o_send[h, zh, core]
                s_recv[h, zh, core] = s_send[h, zh]

    rows = CHIPS * ROWS
    mine = lax.broadcasted_iota(jnp.int32, (rows, SPAN), 1) == core * rows + lax.broadcasted_iota(
        jnp.int32, (rows, SPAN), 0
    )
    for h in range(2):
        for dz in (0, 1, 3, 2):
            zs = (zh + dz) % ZN
            for dc in range(2):
                cs = (core + dc) % 2
                if dz or dc:
                    slot = 8 * h + 2 * zs + cs
                    remote(o_recv.at[h, zs, cs], o_recv.at[h, zs, cs], ot_send.at[0], ot_recv.at[slot], sibling).wait_recv()
                    remote(s_recv.at[h, zs, cs], s_recv.at[h, zs, cs], st_send.at[0], st_recv.at[slot], sibling).wait_recv()
        for cs in range(2):
            lses = [
                jnp.sum(jnp.where(mine, s_recv[h, zs, cs], 0.0), axis=1, keepdims=True) for zs in range(ZN)
            ]
            best = jnp.maximum(jnp.maximum(lses[0], lses[1]), jnp.maximum(lses[2], lses[3]))
            shares = [jnp.exp2(value - best) for value in lses]
            whole = shares[0] + shares[1] + shares[2] + shares[3]
            summed = sum(shares[zs] * o_recv[h, zs, cs].astype(F32) for zs in range(ZN))
            att[:, (2 * cs + h) * HD : (2 * cs + h + 1) * HD] = (summed / whole).astype(BF16)

    remote(w_o.at[other], w_o.at[other], wo_send, wo_recv, sibling).wait_recv()
    def halves(part, side):
        return pl.ds(part * WIDTH + side * (WIDTH // 2), WIDTH // 2)

    for part in range(PARTS):
        cols = pl.ds(part * WIDTH, WIDTH)
        for n in range(WIDTH // 256):
            sub = pl.ds(part * WIDTH + n * 256, 256)
            value = jnp.dot(att[:, : 2 * HD], w_o[0, :, sub], preferred_element_type=F32) + jnp.dot(
                att[:, 2 * HD :], w_o[1, :, sub], preferred_element_type=F32
            )
            p_send[:, :, sub] = value.reshape(CHIPS, ROWS, 256).astype(BF16)
        for dl in range(2):
            for side in range(2):
                n = 4 * part + 2 * dl + side
                send(
                    p_send.at[chip_at(dl, 2), :, halves(part, side)], hop_recv.at[n],
                    hop_send_sem.at[n], hop_recv_sem.at[n], chip_device(0, 1 if side == 0 else 3, core),
                )
        for dl in range(2):
            for side in range(2):
                half = halves(part, 1 - side)
                dy = 1 if side == 0 else 3
                n = 4 * part + 2 * dl + side
                send(
                    p_send.at[chip_at(dl, dy), :, half], p_recv.at[chip, :, half],
                    dir_send.at[n], dir_recv.at[n], chip_device(dl, dy, core),
                )
        send(
            p_send.at[chip_at(1, 0), :, cols], p_recv.at[chip, :, cols], mate_send.at[part], mate_recv.at[part],
            chip_device(1, 0, core),
        )

    for part in range(PARTS):
        for dl in range(2):
            for side in range(2):
                half = halves(part, side)
                n = 4 * part + 2 * dl + side
                held = hop_recv.at[n]
                remote(held, held, hop_send_sem.at[0], hop_recv_sem.at[n], sibling).wait_recv()
                dy = 1 if side == 0 else 3
                index = chip_at(dl, dy)
                added = p_send[index, :, half].astype(F32) + held[...].astype(F32)
                p_sum[n] = added.astype(BF16)
                send(
                    p_sum.at[n], p_recv.at[chip, :, half], sum_send.at[n], sum_recv.at[n], chip_device(dl, dy, core),
                )

    gate = mod[2, pl.ds(level, 1), :]
    for part in range(PARTS):
        cols = pl.ds(part * WIDTH, WIDTH)
        total = p_send[chip, :, cols].astype(F32)
        mate = p_recv.at[chip_at(1, 0), :, cols]
        remote(mate, mate, mate_send.at[0], mate_recv.at[part], sibling).wait_recv()
        total = total + mate[...].astype(F32)
        for dl in range(2):
            for side in range(2):
                source = chip_at(dl, 3 if side == 0 else 1)
                n = 4 * part + 2 * dl + side
                late = p_recv.at[source, :, halves(part, side)]
                early = p_recv.at[source, :, halves(part, 1 - side)]
                remote(early, early, dir_send.at[0], dir_recv.at[n], sibling).wait_recv()
                remote(late, late, sum_send.at[0], sum_recv.at[n], sibling).wait_recv()
                total = total + p_recv[source, :, cols].astype(F32)
        out_ref[:, cols] = (gate[:, part * WIDTH : (part + 1) * WIDTH] * total).astype(BF16)

    for copy in waits:
        copy.wait_send()


def body(
    latents, modulation, w_query, w_key, w_value, w_out, cache_k, cache_v, level_index, rotation, cached_tokens
):
    anywhere = pl.BlockSpec(memory_space=pltpu.HBM)
    dma = pltpu.SemaphoreType.DMA
    rows = CHIPS * ROWS
    return pl.pallas_call(
        kernel,
        out_shape=jax.ShapeDtypeStruct((ROWS, D), BF16),
        in_specs=[anywhere] * 11,
        out_specs=pl.BlockSpec(memory_space=pltpu.VMEM),
        scratch_shapes=[
            pltpu.SMEM((1,), jnp.int32),
            pltpu.SMEM((16,), jnp.int32),
            pltpu.SMEM((1,), jnp.int32),
            pltpu.VMEM((16, ROWS, D), BF16),
            pltpu.VMEM((SPAN, D), BF16),
            pltpu.VMEM((3, 4, D), F32),
            pltpu.VMEM((ROWS, D), F32),
            pltpu.VMEM((ROWS, D), F32),
            pltpu.VMEM((3, D, 2 * HD), BF16),
            pltpu.VMEM((2, 2 * HD, D), BF16),
            pltpu.VMEM((XN, CACHE, 2 * HD), BF16),
            pltpu.VMEM((XN, 2 * HD, CACHE), BF16),
            pltpu.VMEM((2, XN, SPAN, HD), BF16),
            pltpu.VMEM((2, XN, HD, SPAN), BF16),
            pltpu.VMEM((2, ZN, SPAN, HD), BF16),
            pltpu.VMEM((XN * CACHE, SPAN), F32),
            pltpu.VMEM((ZN, XN, ROWS, SPAN), F32),
            pltpu.VMEM((CACHE, 2 * HD), BF16),
            pltpu.VMEM((KEYS, 2 * SPAN), F32),
            pltpu.VMEM((KEYS, 2 * SPAN), BF16),
            pltpu.VMEM((2, ZN, 2, rows, HD), BF16),
            pltpu.VMEM((2, ZN, 2, rows, HD), BF16),
            pltpu.VMEM((2, ZN, 1, SPAN), F32),
            pltpu.VMEM((2, ZN, 2, 1, SPAN), F32),
            pltpu.VMEM((rows, 4 * HD), BF16),
            pltpu.VMEM((CHIPS, ROWS, D), BF16),
            pltpu.VMEM((CHIPS, ROWS, D), BF16),
            pltpu.VMEM((4 * PARTS, ROWS, WIDTH // 2), BF16),
            pltpu.VMEM((4 * PARTS, ROWS, WIDTH // 2), BF16),
            dma((11,)),
            dma((5,)),
            dma((16,)),
            dma((4,)),
            dma((4,)),
            dma((8,)),
            dma((6,)),
            dma((8,)),
            dma((6,)),
            dma((8,)),
            dma((12,)),
            dma((16,)),
            dma(()),
            dma(()),
            dma((14,)),
            dma((16,)),
            dma((14,)),
            dma((16,)),
            dma((4 * PARTS,)),
            dma((4 * PARTS,)),
            dma((4 * PARTS,)),
            dma((4 * PARTS,)),
            dma((4 * PARTS,)),
            dma((4 * PARTS,)),
            dma((PARTS,)),
            dma((PARTS,)),
        ],
        compiler_params=pltpu.CompilerParams(
            collective_id=0, has_side_effects=True, vmem_limit_bytes=60 * 1024 * 1024
        ),
        name="attention_step",
    )(latents, jnp.transpose(modulation, (1, 0, 2)), w_query, w_key, w_value, w_out, cache_k, cache_v, level_index, rotation, cached_tokens)


def solution(mesh):
    placed = (
        P(("span", "tensor"), None),
        P(),
        P(None, "tensor"),
        P(None, "tensor"),
        P(None, "tensor"),
        P("tensor", None),
        P("span", "tensor"),
        P("span", "tensor"),
        P("span"),
        P(),
        P(),
    )
    return jax.shard_map(
        body, mesh=mesh, in_specs=placed, out_specs=P(("span", "tensor"), None), check_vma=False
    )
```
